32 devices in a mesh: ch: 4 (over z), sx: 4 (over x, core), sy: 2 (over y).
Axes of the slice: x: 2, y: 2, z: 4, core: 2. Of those that a mesh axis runs over, the one named last changes fastest.
Arguments:
- inputs: bfloat16 [768, 16, 4, 64], P('ch', 'sx', 'sy'), may hold values from -6 to 6
- pre_act: bfloat16 [768, 16, 4, 64], P('ch', 'sx', 'sy'), may hold values from -6 to 6
- out_grad: bfloat16 [768, 16, 4, 64], P('ch', 'sx', 'sy'), may hold values from -6 to 6
- weight_one: bfloat16 [27, 768, 768], P(None, 'ch'), may hold values from -0.0390625 to 0.0390625
- weight_two: bfloat16 [27, 768, 768], P(None, 'ch'), may hold values from -0.0390625 to 0.0390625
Outputs:
- input_grad: bfloat16 [768, 16, 4, 64], P('ch', 'sx', 'sy')
- filter_one_grad: float32 [27, 768, 768], P(None, 'ch')
- filter_two_grad: float32 [27, 768, 768], P(None, 'ch')
The draws below stay inside these ranges and needn't reach their ends.
All inputs are finite; a program needn't handle non-finite values.
Results may differ from the reference program's by a relative error of at most 0.0049.
Values may be sent and summed in bfloat16 or wider, within the bound.
A program may use at most 192 MiB of HBM per device.

```python
import math
import jax
import jax.numpy as jnp
from jax import lax

C = 768
NX = 16
NY = 4
NZ = 64


def block_levels(stream_key, extent, pieces, smallest, top_value):
    gain, own = 1.0, jax.random.fold_in(stream_key, 6)
    for dim, parts in pieces:
        steps = jnp.exp(jax.random.uniform(jax.random.fold_in(own, dim), (parts,), jnp.float32, smallest / len(pieces), top_value / len(pieces)))
        gain = gain * jnp.repeat(steps, extent[dim] // parts).reshape([-1 if axis == dim else 1 for axis in range(len(extent))])
    return gain


def scatter_about(own_key, extent, width, bound, shards=(), held_as=jnp.bfloat16):
    values = width * jax.random.normal(own_key, extent, jnp.float32)
    if shards:
        values = values * block_levels(own_key, extent, shards, -0.22, 0.18)
    return jnp.clip(values, -bound, bound).astype(held_as)


def setup_inputs(seed: int = 0) -> dict:
    seeds = jax.random.split(jax.random.key(seed), 6)
    return {
        "inputs": scatter_about(seeds[0], (C, NX, NY, NZ), 1.0, 6.0, ((0, 4), (1, 4), (2, 2))),
        "pre_act": scatter_about(seeds[1], (C, NX, NY, NZ), 1.0, 6.0, ((0, 4), (1, 4), (2, 2))),
        "out_grad": scatter_about(seeds[2], (C, NX, NY, NZ), 1.0, 6.0, ((0, 4), (1, 4), (2, 2))),
        "weight_one": scatter_about(seeds[3], (27, C, C), (27 * C) ** -0.5, 0.0390625, ((1, 4),)),
        "weight_two": scatter_about(seeds[4], (27, C, C), (27 * C) ** -0.5, 0.0390625, ((1, 4),)),
    }


def window(padded, offset, mirror):
    first = offset // 9
    second = offset // 3 % 3
    third = offset % 3
    if mirror:
        first, second, third = (2 - first, 2 - second, 2 - third)
    part = padded[:, first:first + NX, second:second + NY, third:third + NZ]
    return part.reshape(C, NX * NY * NZ)

def pad_all(array):
    return jnp.pad(array, ((0, 0), (1, 1), (1, 1), (1, 1)))

def contract_positions(left, right):
    return lax.dot_general(left, right, (((1,), (1,)), ((), ())), preferred_element_type=jnp.float32)

def reference(inputs, pre_act, out_grad, weight_one, weight_two):
    positions = NX * NY * NZ
    inputs_pad = pad_all(inputs)
    grad_pad = pad_all(out_grad)
    active_pad = pad_all(jnp.maximum(pre_act, jnp.zeros((), pre_act.dtype)))
    grad_flat = out_grad.reshape(C, positions)
    act_grad = jnp.zeros((C, positions), jnp.float32)
    filter_two = []
    for offset in range(27):
        act_grad = act_grad + jnp.dot(weight_two[offset], window(grad_pad, offset, True), preferred_element_type=jnp.float32)
        filter_two.append(contract_positions(window(active_pad, offset, False), grad_flat))
    delta = jnp.where(pre_act.reshape(C, positions) > 0, act_grad, 0.0).astype(jnp.bfloat16)
    delta_pad = pad_all(delta.reshape(C, NX, NY, NZ))
    input_grad = jnp.zeros((C, positions), jnp.float32)
    filter_one = []
    for offset in range(27):
        input_grad = input_grad + lax.dot_general(weight_one[offset], window(delta_pad, offset, True), (((0,), (0,)), ((), ())), preferred_element_type=jnp.float32)
        filter_one.append(contract_positions(delta, window(inputs_pad, offset, False)))
    factor = 1.0 / math.sqrt(positions)
    return (input_grad.reshape(C, NX, NY, NZ).astype(jnp.bfloat16), jnp.stack(filter_one) * factor, jnp.stack(filter_two) * factor)
```

```python
import functools
import math

import jax
import jax.numpy as jnp
from jax import lax
from jax.experimental import pallas as pl
from jax.experimental.pallas import tpu as pltpu
from jax.sharding import PartitionSpec as P


def padded_2(cells, sides, width):
    for axis, dim in sides:
        count = lax.axis_size(axis)
        ends = count - 1
        head = lax.slice_in_dim(cells, 0, width, axis=dim)
        tail = lax.slice_in_dim(cells, cells.shape[dim] - width, cells.shape[dim], axis=dim)
        cells = jnp.concatenate(
            [
                lax.ppermute(tail, axis, [(i, (i + 1) % count) for i in range(ends)]),
                cells,
                lax.ppermute(head, axis, [((i + 1) % count, i) for i in range(ends)]),
            ],
            axis=dim,
        )
    return cells


def window(padded, offset, mirror):
    first = offset // 9
    second = offset // 3 % 3
    third = offset % 3
    if mirror:
        first, second, third = (2 - first, 2 - second, 2 - third)
    size_x = padded.shape[1] - 2
    size_y = padded.shape[2] - 2
    size_z = padded.shape[3] - 2
    part = padded[:, first : first + size_x, second : second + size_y, third : third + size_z]
    return part.reshape(padded.shape[0], size_x * size_y * size_z)


def pad_depth(array):
    return jnp.pad(array, ((0, 0), (0, 0), (0, 0), (1, 1)))


def contract_positions(left, right):
    return lax.dot_general(
        left, right, (((1,), (1,)), ((), ())), preferred_element_type=jnp.float32
    )


def contract_first(left, right):
    return lax.dot_general(
        left, right, (((0,), (0,)), ((), ())), preferred_element_type=jnp.float32
    )


def spread_flat(array):
    padded = jnp.pad(array, ((0, 0), (0, 0), (0, 1), (0, 1)))
    return padded.reshape(padded.shape[0], -1)


def whole_window(blocks, counts):
    count_x, count_y = counts
    channels, size_x, size_y, size_z = blocks.shape[1:]
    grid = blocks.reshape(count_x, count_y, channels, size_x, size_y, size_z)
    grid = grid.transpose(2, 0, 3, 1, 4, 5)
    return grid.reshape(channels, count_x * size_x, count_y * size_y, size_z)


def column_slices(full, counts):
    ranks = counts[0] * counts[1]
    cut = full.reshape(ranks, full.shape[0] // ranks, *full.shape[1:])
    return whole_window(lax.all_to_all(cut, ("sx", "sy"), 0, 0, tiled=True), counts)


def shifts(size_y, size_z):
    row = size_z + 1
    plane = (size_y + 1) * row
    return [
        (a - 1) * plane + (b - 1) * row + c - 1
        for a in range(3)
        for b in range(3)
        for c in range(3)
    ]


def filter_slice(rows, columns, shift_rows):
    steps = shifts(rows.shape[2], rows.shape[3])
    margin = max(steps)
    left = spread_flat(rows)
    size = left.shape[1]
    right = jnp.pad(spread_flat(columns), ((0, 0), (margin, margin)))
    out = []
    for step in steps:
        start = margin - step if shift_rows else margin + step
        part = lax.slice_in_dim(right, start, start + size, axis=1)
        out.append(contract_positions(left, part))
    return jnp.stack(out)


def join_columns(part, factor):
    sent = (part * factor).astype(jnp.bfloat16)
    parts = lax.all_gather(sent, ("sx", "sy"), axis=0)
    return jnp.concatenate([parts[i] for i in range(parts.shape[0])], axis=2).astype(jnp.float32)


def shards(inputs, pre_act, out_grad, weight_one, weight_two):
    shape = pre_act.shape
    positions = shape[1] * shape[2] * shape[3]
    counts = (lax.axis_size("sx"), lax.axis_size("sy"))
    factor = 1.0 / math.sqrt(positions * counts[0] * counts[1])
    full_grad = lax.all_gather(out_grad, "ch", axis=0, tiled=True)
    active = jnp.maximum(pre_act, jnp.zeros((), pre_act.dtype))
    active_all = whole_window(lax.all_gather(active, ("sx", "sy"), axis=0), counts)
    grad_columns = column_slices(full_grad, counts)
    grad_pad = pad_depth(padded_2(full_grad, (("sx", 1), ("sy", 2)), 1))
    filter_two = join_columns(filter_slice(active_all, grad_columns, True), factor)
    act_grad = jnp.zeros((shape[0], positions), jnp.float32)
    for offset in range(27):
        act_grad = act_grad + jnp.dot(
            weight_two[offset], window(grad_pad, offset, True), preferred_element_type=jnp.float32
        )
    delta = jnp.where(pre_act.reshape(shape[0], positions) > 0, act_grad, 0.0).astype(jnp.bfloat16)
    delta = delta.reshape(shape)
    full_in = lax.all_gather(inputs, "ch", axis=0, tiled=True)
    input_columns = column_slices(full_in, counts)
    delta_all = whole_window(lax.all_gather(delta, ("sx", "sy"), axis=0), counts)
    filter_one = join_columns(filter_slice(delta_all, input_columns, False), factor)
    delta_pad = pad_depth(padded_2(delta, (("sx", 1), ("sy", 2)), 1))
    partial_terms = jnp.zeros((weight_one.shape[2], positions), jnp.float32)
    for offset in range(27):
        partial_terms = partial_terms + contract_first(
            weight_one[offset], window(delta_pad, offset, True)
        )
    partial_terms = partial_terms.reshape(weight_one.shape[2], shape[1], shape[2], shape[3])
    input_grad = lax.psum_scatter(partial_terms, "ch", scatter_dimension=0, tiled=True).astype(
        jnp.bfloat16
    )
    return (input_grad, filter_one, filter_two)


F32 = jnp.float32
BF16 = jnp.bfloat16
MESH = pl.DeviceIdType.MESH
ANY = pl.BlockSpec(memory_space=pl.ANY)
IN_VMEM = pl.BlockSpec(memory_space=pltpu.VMEM)


def dot_lanes(left, right):
    return lax.dot_general(left, right, (((1,), (1,)), ((), ())), preferred_element_type=F32)


def lanes(shape):
    return lax.broadcasted_iota(jnp.int32, shape, len(shape) - 1)


def swap_halves(tile):
    return pltpu.roll(tile, tile.shape[-1] // 2, 1)


class Gather:
    def __init__(self, index, own, slot, half, send, recv, here):
        z, s, y = here
        flip = lax.rem(s + 2, 4)
        other = s + 1 - 2 * lax.rem(s, 2)
        other_flip = lax.rem(other + 2, 4)
        self.near = [(z, flip, y), (z, s, 1 - y), (z, other, y)]
        self.mine, self.from_x, self.from_y, self.from_d = (s, y), (flip, y), (s, 1 - y), (flip, 1 - y)
        self.pair = [(other, y), (other_flip, y), (other, 1 - y), (other_flip, 1 - y)]
        self.index, self.own, self.slot, self.half = index, own, slot, half
        self.send, self.recv = send, recv

    def copy(self, step, src, dst, to):
        return pltpu.make_async_remote_copy(
            src_ref=src,
            dst_ref=dst,
            send_sem=self.send.at[self.index, step],
            recv_sem=self.recv.at[self.index, step],
            device_id=self.near[to],
            device_id_type=MESH,
        )

    def sends(self):
        mine, slot, half = self.slot(self.mine), self.slot, self.half
        return [
            (0, self.own, mine, 0),
            (1, self.own, mine, 1),
            (2, self.own, mine, 2),
            (3, half(self.from_x, 0), half(self.from_x, 0), 1),
            (4, half(self.from_y, 1), half(self.from_y, 1), 0),
            (5, slot(self.from_x), slot(self.from_x), 2),
            (6, slot(self.from_y), slot(self.from_y), 2),
            (7, slot(self.from_d), slot(self.from_d), 2),
        ]

    def begin(self, steps):
        for entry in self.sends():
            if entry[0] in steps:
                self.copy(*entry).start()

    def arrive(self, step):
        where = {
            0: lambda: self.slot(self.from_x),
            1: lambda: self.slot(self.from_y),
            2: lambda: self.slot(self.pair[0]),
            3: lambda: self.half(self.from_d, 0),
            4: lambda: self.half(self.from_d, 1),
            5: lambda: self.slot(self.pair[1]),
            6: lambda: self.slot(self.pair[2]),
            7: lambda: self.slot(self.pair[3]),
        }[step]()
        self.copy(step, where, where, 0).wait_recv()

    def start(self):
        self.begin((0, 1, 2))

    def relay(self):
        self.arrive(0)
        self.begin((3, 5))
        self.arrive(1)
        self.begin((4, 6))

    def relay_far(self):
        self.arrive(3)
        self.arrive(4)
        self.begin((7,))

    def finish(self):
        for step in (2, 5, 6, 7):
            self.arrive(step)

    def drain(self):
        for entry in self.sends():
            self.copy(*entry).wait_send()


def fused_kernel(
    dims, factor,
    g_ref, in_ref, act_ref, w1_hbm, w2_hbm,
    ig_ref, pieces,
    acts, deltas, cols, full, edge, pack_s, pack_r, corner, tall, weight, shifted,
    facc, parts, cacc, dl, dpos, zacc, igt, term_s, term_r,
    ag_s, ag_r, c1_s, c1_r, c1_l, c2_s, c2_r, g_s, g_r, h_s, h_r, t_s, t_r, w_sem, o_sem,
):
    nch, nsx, nsy, rows, lx, ly, nz = dims
    lane = ly * nz
    nk = nsx * nsy
    piece = rows * nch // nk
    sub = piece // 2
    npos = lx * lane
    wide = nsy * lane
    z, s, y = lax.axis_index("ch"), lax.axis_index("sx"), lax.axis_index("sy")
    here = (z, s, y)
    mine = s * nsy + y
    parity = lax.rem(z, 2)
    core = lax.rem(s, 2)
    turn = z // 2

    barrier = pltpu.get_barrier_semaphore()
    for step in range(1, nk):
        k = lax.rem(mine + step, nk)
        pl.semaphore_signal(
            barrier, inc=1, device_id=(z, k // nsy, lax.rem(k, nsy)), device_id_type=MESH
        )
    for step in range(1, nch):
        pl.semaphore_signal(
            barrier, inc=1, device_id=(lax.rem(z + step, nch), s, y), device_id_type=MESH
        )
    pl.semaphore_wait(barrier, nk - 1 + nch - 1)

    load_two = pltpu.make_async_copy(w2_hbm, weight, w_sem.at[0])
    load_two.start()
    load_one = pltpu.make_async_copy(w1_hbm, weight, w_sem.at[1])

    def block_copy(op, ref, q):
        dst_s, dst_y = 2 * (q // 2) + parity, q % 2
        src = ref.at[:, pl.ds(q * sub, sub)]
        dst = cols.at[op, turn, mine]
        remote = pltpu.make_async_remote_copy(
            src_ref=src, dst_ref=dst, send_sem=c1_s.at[op, q], recv_sem=c1_r.at[op, mine],
            device_id=(z, dst_s, dst_y), device_id_type=MESH,
        )
        local = pltpu.make_async_copy(src, dst, c1_l.at[op])
        same = jnp.logical_and(dst_s == s, dst_y == y)
        return same, local, remote

    def blocks_start(op, ref):
        for q in range(nk // 2):
            same, local, remote = block_copy(op, ref, q)

            @pl.when(same)
            def _():
                local.start()

            @pl.when(jnp.logical_not(same))
            def _():
                remote.start()

    def blocks_wait(op, ref):
        @pl.when(parity == core)
        def _():
            for step in range(1, nk):
                k = lax.rem(mine + step, nk)
                dst = cols.at[op, turn, k]
                pltpu.make_async_remote_copy(
                    src_ref=dst, dst_ref=dst, send_sem=c1_s.at[op, 0], recv_sem=c1_r.at[op, k],
                    device_id=here, device_id_type=MESH,
                ).wait_recv()
        for q in range(nk // 2):
            same, local, remote = block_copy(op, ref, q)

            @pl.when(same)
            def _():
                local.wait()

    def blocks_drain(op, ref):
        for q in range(nk // 2):
            same, local, remote = block_copy(op, ref, q)

            @pl.when(jnp.logical_not(same))
            def _():
                remote.wait_send()

    def spread_copy(op, step):
        block = cols.at[op, turn]
        return pltpu.make_async_remote_copy(
            src_ref=block, dst_ref=block, send_sem=c2_s.at[op, step - 1], recv_sem=c2_r.at[op, turn],
            device_id=(lax.rem(z + step, nch), s, y), device_id_type=MESH,
        )

    def spread_start(op):
        @pl.when(parity == core)
        def _():
            for step in range(1, nch):
                spread_copy(op, step).start()

    def spread_wait(op):
        for t in range(2):
            @pl.when(core + 2 * t != z)
            def _():
                block = cols.at[op, t]
                pltpu.make_async_remote_copy(
                    src_ref=block, dst_ref=block, send_sem=c2_s.at[op, 0], recv_sem=c2_r.at[op, t],
                    device_id=here, device_id_type=MESH,
                ).wait_recv()

    def spread_drain(op):
        @pl.when(parity == core)
        def _():
            for step in range(1, nch):
                spread_copy(op, step).wait_send()

    def full_copy(step):
        return pltpu.make_async_remote_copy(
            src_ref=g_ref, dst_ref=full.at[z], send_sem=g_s.at[step - 1], recv_sem=g_r.at[z],
            device_id=(lax.rem(z + step, nch), s, y), device_id_type=MESH,
        )

    def whole(ref):
        slot = lambda k: ref.at[pl.ds(lx * k[0], lx), k[1]]
        half = lambda k, i: ref.at[pl.ds(lx * k[0] + i * (lx // 2), lx // 2), k[1]]
        return slot, half

    act_gather = Gather(0, act_ref, *whole(acts), ag_s, ag_r, here)
    delta_gather = Gather(1, dl, *whole(deltas), ag_s, ag_r, here)
    size = parts.shape[3]
    cut = size // 2 // 16 * 16

    def piece_gather(which, n):
        slot = lambda k: parts.at[which, n, k[0] * nsy + k[1]]
        half = lambda k, i: parts.at[
            which, n, k[0] * nsy + k[1], pl.ds(0, cut) if i == 0 else pl.ds(cut, size - cut)
        ]
        return Gather(2 + 9 * which + n, slot((s, y)), slot, half, ag_s, ag_r, here)

    blocks_start(0, g_ref)
    act_gather.start()
    blocks_start(1, in_ref)
    acts[pl.ds(lx * s, lx), y] = act_ref[...]
    full[z] = g_ref[...]
    blocks_wait(0, g_ref)
    spread_start(0)
    for step in range(1, nch):
        full_copy(step).start()
    act_gather.relay()
    blocks_wait(1, in_ref)
    spread_start(1)
    act_gather.relay_far()

    shifted[0] = jnp.zeros(shifted.shape[1:], BF16)
    shifted[shifted.shape[0] - 1] = jnp.zeros(shifted.shape[1:], BF16)

    def shift_columns(op):
        @pl.loop(0, nsx * lx)
        def _(p):
            owner, inner = p // lx, lax.rem(p, lx)
            tiles = [
                jnp.concatenate([cols[op, t, owner * nsy + j, inner] for t in range(2)], axis=0)
                for j in range(nsy)
            ]
            plane = jnp.concatenate(tiles, axis=1).astype(F32)
            where = lanes((piece, wide))
            row, depth = where // nz, lax.rem(where, nz)
            for b in range(3):
                for c in range(3):
                    move = (nz * (b - 1) + c - 1) % wide
                    value = pltpu.roll(plane, move, 1) if move else plane
                    keep = where >= 0
                    if b == 0:
                        keep = jnp.logical_and(keep, row < nsy * ly - 1)
                    if b == 2:
                        keep = jnp.logical_and(keep, row > 0)
                    if c == 0:
                        keep = jnp.logical_and(keep, depth < nz - 1)
                    if c == 2:
                        keep = jnp.logical_and(keep, depth > 0)
                    value = jnp.where(keep, value, 0.0).astype(BF16)
                    start = (3 * b + c) * piece
                    for j in range(nsy):
                        shifted[p + 1, j, pl.ds(start, piece)] = value[:, j * lane : (j + 1) * lane]

    def filter_pieces(which, left, first, last):
        @pl.loop(first, last)
        def _(a):
            facc[:, :rows] = jnp.zeros((facc.shape[0], rows), F32)

            @pl.loop(0, nsx)
            def _(o):
                cells = shifted[pl.ds(2 - a + lx * o, lx)]
                other = left[pl.ds(lx * o, lx)]
                cells = jnp.concatenate([cells[i, j] for i in range(lx) for j in range(nsy)], axis=1)
                other = jnp.concatenate([other[i, j] for i in range(lx) for j in range(nsy)], axis=1)
                facc[:, :rows] += dot_lanes(cells, other)

            group = 3 * piece
            for b in range(3):
                n = 3 * a + b
                main = facc[pl.ds(group * b, group), :lane] * factor
                parts[which, n, mine, pl.ds(0, group)] = main.astype(BF16)
                low = facc[pl.ds(group * b, group // 2), lane : 2 * lane] * factor
                high = facc[pl.ds(group * b + group // 2, group // 2), lane : 2 * lane] * factor
                both = jnp.where(lanes(low.shape) < rows - lane, low, swap_halves(high))
                parts[which, n, mine, pl.ds(group, group // 2)] = both.astype(BF16)
                piece_gather(which, n).start()

    def relay_pieces(which, first, last):
        @pl.loop(first, last)
        def _(n):
            piece_gather(which, n).relay()

    def write_piece(which, n):
        return pltpu.make_async_copy(parts.at[which, n], pieces.at[which, n], o_sem.at[which, n])

    def finish_pieces(which, first, last):
        @pl.loop(first, last)
        def _(n):
            piece_gather(which, n).relay_far()

        @pl.loop(first, last)
        def _(n):
            piece_gather(which, n).finish()
            write_piece(which, n).start()

    facc[...] = jnp.zeros(facc.shape, F32)
    act_gather.finish()
    spread_wait(0)
    shift_columns(0)
    filter_pieces(0, acts, 0, 3)

    for step in range(1, nch):
        k = lax.rem(z + step, nch)
        pltpu.make_async_remote_copy(
            src_ref=full.at[k], dst_ref=full.at[k], send_sem=g_s.at[0], recv_sem=g_r.at[k],
            device_id=here, device_id_type=MESH,
        ).wait_recv()

    low_half = lanes((rows, lane)) < nz
    for k in range(nch):
        for pair in range(lx // 2):
            first = full[k, 2 * pair].astype(F32)
            second = full[k, 2 * pair + 1].astype(F32)
            low = jnp.where(y == 0, swap_halves(first), first)
            high = jnp.where(y == 0, second, swap_halves(second))
            pack_s[k, pair] = jnp.where(low_half, low, high).astype(BF16)

    left_dev = (z, lax.rem(s + nsx - 1, nsx), y)
    right_dev = (z, lax.rem(s + 1, nsx), y)

    def halo(i, src, dst, dev):
        return pltpu.make_async_remote_copy(
            src_ref=src, dst_ref=dst, send_sem=h_s.at[i], recv_sem=h_r.at[i],
            device_id=dev, device_id_type=MESH,
        )

    to_y = halo(0, pack_s, pack_r, (z, s, 1 - y))
    to_left = halo(1, full.at[:, 0], edge.at[1], left_dev)
    to_right = halo(2, full.at[:, lx - 1], edge.at[0], right_dev)
    corner_left = halo(3, pack_r.at[:, 0], corner.at[1], left_dev)
    corner_right = halo(4, pack_r.at[:, lx // 2 - 1], corner.at[0], right_dev)
    has_left, has_right = s > 0, s < nsx - 1
    to_y.start()

    @pl.when(has_left)
    def _():
        to_left.start()

    @pl.when(has_right)
    def _():
        to_right.start()

    to_y.wait_recv()

    @pl.when(has_left)
    def _():
        corner_left.start()

    @pl.when(has_right)
    def _():
        corner_right.start()

    relay_pieces(0, 0, 9)

    @pl.when(has_right)
    def _():
        to_left.wait_recv()
        corner_left.wait_recv()

    @pl.when(has_left)
    def _():
        to_right.wait_recv()
        corner_right.wait_recv()

    for x in range(lx + 2):
        for k in range(nch):
            if x == 0:
                tile = jnp.where(has_left, edge[0, k].astype(F32), 0.0)
                beside = jnp.where(has_left, corner[0, k].astype(F32), 0.0)
                upper = True
            elif x == lx + 1:
                tile = jnp.where(has_right, edge[1, k].astype(F32), 0.0)
                beside = jnp.where(has_right, corner[1, k].astype(F32), 0.0)
                upper = False
            else:
                tile = full[k, x - 1].astype(F32)
                beside = pack_r[k, (x - 1) // 2].astype(F32)
                upper = (x - 1) % 2 == 1
            turned = swap_halves(beside)
            in_low, in_high = (turned, beside) if upper else (beside, turned)
            swapped = swap_halves(tile)
            above = jnp.where(low_half, swapped, jnp.where(y == 0, in_high, 0.0))
            below = jnp.where(low_half, jnp.where(y == 0, 0.0, in_low), swapped)
            tall[0, x, pl.ds(k * rows, rows)] = above.astype(BF16)
            tall[1, x, pl.ds(k * rows, rows)] = tile.astype(BF16)
            tall[2, x, pl.ds(k * rows, rows)] = below.astype(BF16)

    load_two.wait()
    cacc[...] = jnp.zeros(cacc.shape, F32)

    @pl.loop(0, 9)
    def _(ab):
        a, b = ab // 3, lax.rem(ab, 3)
        left = weight[pl.ds(3 * ab, 3)].reshape(3 * rows, nch * rows)
        right = tall[b, pl.ds(2 - a, lx)]
        right = jnp.concatenate([right[i] for i in range(lx)], axis=1)
        cacc[...] += jnp.dot(left, right, preferred_element_type=F32)

    load_one.start()
    depth = lax.rem(lanes((rows, lane)), nz)
    for x in range(lx):
        cut_x = slice(x * lane, (x + 1) * lane)
        total = cacc[rows : 2 * rows, cut_x]
        total += jnp.where(depth < nz - 1, pltpu.roll(cacc[:rows, cut_x], lane - 1, 1), 0.0)
        total += jnp.where(depth > 0, pltpu.roll(cacc[2 * rows :, cut_x], 1, 1), 0.0)
        total = jnp.where(act_ref[x].astype(F32) > 0.0, total, 0.0).astype(BF16)
        dl[x] = total
        deltas[lx * s + x, y] = total
    delta_gather.start()

    finish_pieces(0, 0, 9)
    spread_wait(1)
    shift_columns(1)
    delta_gather.relay()
    delta_gather.relay_far()
    delta_gather.finish()
    filter_pieces(1, deltas, 0, 3)

    for x in range(lx + 2):
        place = lx * s + x - 1
        inside = jnp.logical_and(place >= 0, place < nsx * lx)
        place = jnp.clip(place, 0, nsx * lx - 1)
        own = deltas[place, y].astype(F32).T
        beside = deltas[place, 1 - y].astype(F32).T
        own = jnp.where(inside, own, 0.0).astype(BF16)
        beside = jnp.where(inside, jnp.where(y == 0, beside[:nz], beside[lane - nz :]), 0.0)
        dpos[x, 0] = jnp.where(y == 0, 0.0, beside).astype(BF16)
        for j in range(ly):
            dpos[x, 1 + j] = own[j * nz : (j + 1) * nz]
        dpos[x, ly + 1] = jnp.where(y == 0, beside, 0.0).astype(BF16)

    zacc[...] = jnp.zeros(zacc.shape, F32)
    load_one.wait()

    @pl.loop(0, 9)
    def _(ab):
        a, b = ab // 3, lax.rem(ab, 3)
        left = dpos[pl.ds(2 - a, lx), pl.ds(2 - b, ly)].reshape(npos, rows)
        for c in range(3):
            zacc[c] += jnp.dot(left, weight[3 * ab + c], preferred_element_type=F32)

    for i in range(npos // nz):
        span = slice(i * nz, (i + 1) * nz)
        total = zacc[1, span]
        at = lax.broadcasted_iota(jnp.int32, total.shape, 0)
        total += jnp.where(at < nz - 1, pltpu.roll(zacc[0, span], nz - 1, 0), 0.0)
        total += jnp.where(at > 0, pltpu.roll(zacc[2, span], 1, 0), 0.0)
        igt[span] = total.astype(BF16)

    for k in range(nch):
        shape = (rows, nch * rows)
        pick = lanes(shape) == lax.broadcasted_iota(jnp.int32, shape, 0) + k * rows
        value = dot_lanes(pick.astype(BF16), igt[...]).astype(BF16)
        for x in range(lx):
            term_s[k, x] = value[:, x * lane : (x + 1) * lane]

    def term_copy(step):
        to = lax.rem(z + step, nch)
        return pltpu.make_async_remote_copy(
            src_ref=term_s.at[to], dst_ref=term_r.at[z], send_sem=t_s.at[step - 1],
            recv_sem=t_r.at[z], device_id=(to, s, y), device_id_type=MESH,
        )

    for step in range(1, nch):
        term_copy(step).start()
    relay_pieces(1, 0, 9)
    finish_pieces(1, 0, 9)

    total = term_s[z].astype(F32)
    for step in range(1, nch):
        k = lax.rem(z + step, nch)
        pltpu.make_async_remote_copy(
            src_ref=term_r.at[k], dst_ref=term_r.at[k], send_sem=t_s.at[0], recv_sem=t_r.at[k],
            device_id=here, device_id_type=MESH,
        ).wait_recv()
        total += term_r[k].astype(F32)
    ig_ref[...] = total.astype(BF16)

    for op, ref in ((0, g_ref), (1, in_ref)):
        blocks_drain(op, ref)
        spread_drain(op)
    for step in range(1, nch):
        full_copy(step).wait_send()
        term_copy(step).wait_send()
    to_y.wait_send()

    @pl.when(has_left)
    def _():
        to_left.wait_send()
        corner_left.wait_send()

    @pl.when(has_right)
    def _():
        to_right.wait_send()
        corner_right.wait_send()

    act_gather.drain()
    delta_gather.drain()
    for which in range(2):
        @pl.loop(0, 9)
        def _(n):
            piece_gather(which, n).drain()
            write_piece(which, n).wait()


def join_kernel(dims, two_ref, one_ref, out_two, out_one):
    nch, nsx, nsy, rows, lx, ly, nz = dims
    lane = ly * nz
    nk = nsx * nsy
    piece = rows * nch // nk
    sub = piece // 2
    group = 3 * piece
    rest = rows - lane
    shape = (lane, lane)
    same = (lanes(shape) == lax.broadcasted_iota(jnp.int32, shape, 0)).astype(BF16)
    shape = (rest, lane)
    down = lax.broadcasted_iota(jnp.int32, shape, 0)
    picks = [(lanes(shape) == down + i * rest).astype(BF16) for i in range(2)]
    for ref, out, mirror in ((two_ref, out_two, False), (one_ref, out_one, True)):
        for c in range(3):
            to = 2 - c if mirror else c
            main, tail = [], []
            for k in range(nch):
                for q in range(nk // 2):
                    slot = (2 * (q // 2) + k % 2) * nsy + q % 2
                    row = c * piece + (k // 2) * sub
                    main.append(ref[slot, row : row + sub])
                    row = group + (row if row < group // 2 else row - group // 2)
                    tail.append(ref[slot, row : row + sub])
            half = len(main) // 2
            for i in range(2):
                span = slice(i * half * sub, (i + 1) * half * sub)
                part = jnp.concatenate(main[i * half : (i + 1) * half], axis=0)
                out[to, :lane, span] = dot_lanes(same, part)
                part = jnp.concatenate(tail[i * half : (i + 1) * half], axis=0)
                upper = c * piece + i * sub >= group // 2
                out[to, lane:, span] = dot_lanes(picks[1 if upper else 0], part)


def tiles(array):
    rows, lx, ly, nz = array.shape
    return array.reshape(rows, lx, ly * nz).transpose(1, 0, 2)


def fused_shards(inputs, pre_act, out_grad, weight_one, weight_two):
    rows, lx, ly, nz = pre_act.shape
    nch, nsx, nsy = (lax.axis_size(axis) for axis in ("ch", "sx", "sy"))
    dims = (nch, nsx, nsy, rows, lx, ly, nz)
    lane = ly * nz
    nk = nsx * nsy
    channels = nch * rows
    piece = channels // nk
    npos = lx * lane
    factor = 1.0 / math.sqrt(npos * nk)
    size = 3 * piece * rows // lane
    planes = nsx * lx
    tile = (lx, rows, lane)
    vm = lambda *shape: pltpu.VMEM(shape, BF16)
    dma = lambda *shape: pltpu.SemaphoreType.DMA(shape)
    active = jnp.maximum(pre_act, jnp.zeros((), pre_act.dtype))
    grad, pieces = pl.pallas_call(
        functools.partial(fused_kernel, dims, factor),
        out_shape=(
            jax.ShapeDtypeStruct(tile, BF16),
            jax.ShapeDtypeStruct((2, 9, nk, size, lane), BF16),
        ),
        in_specs=[IN_VMEM] * 3 + [ANY] * 2,
        out_specs=(IN_VMEM, ANY),
        scratch_shapes=[
            vm(planes, nsy, rows, lane),
            vm(planes, nsy, rows, lane),
            vm(2, 2, nk, lx, piece // 2, lane),
            vm(nch, lx, rows, lane),
            vm(2, nch, rows, lane),
            vm(nch, lx // 2, rows, lane),
            vm(nch, lx // 2, rows, lane),
            vm(2, nch, rows, lane),
            vm(3, lx + 2, channels, lane),
            vm(27, rows, channels),
            vm(planes + 2, nsy, 9 * piece, lane),
            pltpu.VMEM((9 * piece, 2 * lane), F32),
            vm(2, 9, nk, size, lane),
            pltpu.VMEM((3 * rows, npos), F32),
            vm(lx, rows, lane),
            vm(lx + 2, ly + 2, nz, rows),
            pltpu.VMEM((3, npos, channels), F32),
            vm(npos, channels),
            vm(nch, lx, rows, lane),
            vm(nch, lx, rows, lane),
            dma(20, 8), dma(20, 8), dma(2, nk // 2), dma(2, nk), dma(2),
            dma(2, nch - 1), dma(2, 2), dma(nch - 1), dma(nch),
            dma(5), dma(5), dma(nch - 1), dma(nch), dma(2), dma(2, 9),
        ],
        compiler_params=pltpu.CompilerParams(
            collective_id=0, has_side_effects=True, vmem_limit_bytes=62 * 1024 * 1024
        ),
    )(tiles(out_grad), tiles(inputs), tiles(active), weight_one, weight_two)
    block = (None, None, nk, size, lane)
    two, one = pl.pallas_call(
        functools.partial(join_kernel, dims),
        grid=(9,),
        out_shape=(jax.ShapeDtypeStruct((27, rows, channels), F32),) * 2,
        in_specs=[
            pl.BlockSpec(block, lambda n: (0, n, 0, 0, 0)),
            pl.BlockSpec(block, lambda n: (1, n, 0, 0, 0)),
        ],
        out_specs=(
            pl.BlockSpec((3, rows, channels), lambda n: (n, 0, 0)),
            pl.BlockSpec((3, rows, channels), lambda n: (8 - n, 0, 0)),
        ),
        compiler_params=pltpu.CompilerParams(vmem_limit_bytes=40 * 1024 * 1024),
    )(pieces, pieces)
    grad = grad.transpose(1, 0, 2).reshape(rows, lx, ly, nz)
    return grad, one, two


def fits(mesh, rows, lx, ly, nz):
    nch, nsx, nsy = (mesh.shape[axis] for axis in ("ch", "sx", "sy"))
    return (
        (nch, nsx, nsy) == (4, 4, 2)
        and lx % 4 == 0
        and ly == 2
        and ly * nz == 128
        and rows % 64 == 0
        and 128 < rows < 256
    )


def solution(mesh):
    in_specs = (
        P("ch", "sx", "sy", None),
        P("ch", "sx", "sy", None),
        P("ch", "sx", "sy", None),
        P(None, "ch", None),
        P(None, "ch", None),
    )
    out_specs = (P("ch", "sx", "sy", None), P(None, "ch", None), P(None, "ch", None))

    def body(*args):
        return (fused_shards if fits(mesh, *args[1].shape) else shards)(*args)

    return jax.shard_map(body, mesh=mesh, in_specs=in_specs, out_specs=out_specs, check_vma=False)
```

```python
import functools
import math

import jax
import jax.numpy as jnp
from jax import lax
from jax.experimental import pallas as pl
from jax.experimental.pallas import tpu as pltpu
from jax.sharding import PartitionSpec as P


def padded_2(cells, sides, width):
    for axis, dim in sides:
        count = lax.axis_size(axis)
        ends = count - 1
        head = lax.slice_in_dim(cells, 0, width, axis=dim)
        tail = lax.slice_in_dim(cells, cells.shape[dim] - width, cells.shape[dim], axis=dim)
        cells = jnp.concatenate(
            [
                lax.ppermute(tail, axis, [(i, (i + 1) % count) for i in range(ends)]),
                cells,
                lax.ppermute(head, axis, [((i + 1) % count, i) for i in range(ends)]),
            ],
            axis=dim,
        )
    return cells


def window(padded, offset, mirror):
    first = offset // 9
    second = offset // 3 % 3
    third = offset % 3
    if mirror:
        first, second, third = (2 - first, 2 - second, 2 - third)
    size_x = padded.shape[1] - 2
    size_y = padded.shape[2] - 2
    size_z = padded.shape[3] - 2
    part = padded[:, first : first + size_x, second : second + size_y, third : third + size_z]
    return part.reshape(padded.shape[0], size_x * size_y * size_z)


def pad_depth(array):
    return jnp.pad(array, ((0, 0), (0, 0), (0, 0), (1, 1)))


def contract_positions(left, right):
    return lax.dot_general(
        left, right, (((1,), (1,)), ((), ())), preferred_element_type=jnp.float32
    )


def contract_first(left, right):
    return lax.dot_general(
        left, right, (((0,), (0,)), ((), ())), preferred_element_type=jnp.float32
    )


def spread_flat(array):
    padded = jnp.pad(array, ((0, 0), (0, 0), (0, 1), (0, 1)))
    return padded.reshape(padded.shape[0], -1)


def whole_window(blocks, counts):
    count_x, count_y = counts
    channels, size_x, size_y, size_z = blocks.shape[1:]
    grid = blocks.reshape(count_x, count_y, channels, size_x, size_y, size_z)
    grid = grid.transpose(2, 0, 3, 1, 4, 5)
    return grid.reshape(channels, count_x * size_x, count_y * size_y, size_z)


def column_slices(full, counts):
    ranks = counts[0] * counts[1]
    cut = full.reshape(ranks, full.shape[0] // ranks, *full.shape[1:])
    return whole_window(lax.all_to_all(cut, ("sx", "sy"), 0, 0, tiled=True), counts)


def shifts(size_y, size_z):
    row = size_z + 1
    plane = (size_y + 1) * row
    return [
        (a - 1) * plane + (b - 1) * row + c - 1
        for a in range(3)
        for b in range(3)
        for c in range(3)
    ]


def filter_slice(rows, columns, shift_rows):
    steps = shifts(rows.shape[2], rows.shape[3])
    margin = max(steps)
    left = spread_flat(rows)
    size = left.shape[1]
    right = jnp.pad(spread_flat(columns), ((0, 0), (margin, margin)))
    out = []
    for step in steps:
        start = margin - step if shift_rows else margin + step
        part = lax.slice_in_dim(right, start, start + size, axis=1)
        out.append(contract_positions(left, part))
    return jnp.stack(out)


def join_columns(part, factor):
    sent = (part * factor).astype(jnp.bfloat16)
    parts = lax.all_gather(sent, ("sx", "sy"), axis=0)
    return jnp.concatenate([parts[i] for i in range(parts.shape[0])], axis=2).astype(jnp.float32)


def shards(inputs, pre_act, out_grad, weight_one, weight_two):
    shape = pre_act.shape
    positions = shape[1] * shape[2] * shape[3]
    counts = (lax.axis_size("sx"), lax.axis_size("sy"))
    factor = 1.0 / math.sqrt(positions * counts[0] * counts[1])
    full_grad = lax.all_gather(out_grad, "ch", axis=0, tiled=True)
    active = jnp.maximum(pre_act, jnp.zeros((), pre_act.dtype))
    active_all = whole_window(lax.all_gather(active, ("sx", "sy"), axis=0), counts)
    grad_columns = column_slices(full_grad, counts)
    grad_pad = pad_depth(padded_2(full_grad, (("sx", 1), ("sy", 2)), 1))
    filter_two = join_columns(filter_slice(active_all, grad_columns, True), factor)
    act_grad = jnp.zeros((shape[0], positions), jnp.float32)
    for offset in range(27):
        act_grad = act_grad + jnp.dot(
            weight_two[offset], window(grad_pad, offset, True), preferred_element_type=jnp.float32
        )
    delta = jnp.where(pre_act.reshape(shape[0], positions) > 0, act_grad, 0.0).astype(jnp.bfloat16)
    delta = delta.reshape(shape)
    full_in = lax.all_gather(inputs, "ch", axis=0, tiled=True)
    input_columns = column_slices(full_in, counts)
    delta_all = whole_window(lax.all_gather(delta, ("sx", "sy"), axis=0), counts)
    filter_one = join_columns(filter_slice(delta_all, input_columns, False), factor)
    delta_pad = pad_depth(padded_2(delta, (("sx", 1), ("sy", 2)), 1))
    partial_terms = jnp.zeros((weight_one.shape[2], positions), jnp.float32)
    for offset in range(27):
        partial_terms = partial_terms + contract_first(
            weight_one[offset], window(delta_pad, offset, True)
        )
    partial_terms = partial_terms.reshape(weight_one.shape[2], shape[1], shape[2], shape[3])
    input_grad = lax.psum_scatter(partial_terms, "ch", scatter_dimension=0, tiled=True).astype(
        jnp.bfloat16
    )
    return (input_grad, filter_one, filter_two)


F32 = jnp.float32
BF16 = jnp.bfloat16
MESH = pl.DeviceIdType.MESH
ANY = pl.BlockSpec(memory_space=pl.ANY)
IN_VMEM = pl.BlockSpec(memory_space=pltpu.VMEM)


def dot_lanes(left, right):
    return lax.dot_general(left, right, (((1,), (1,)), ((), ())), preferred_element_type=F32)


def lanes(shape):
    return lax.broadcasted_iota(jnp.int32, shape, len(shape) - 1)


def swap_halves(tile):
    return pltpu.roll(tile, tile.shape[-1] // 2, 1)


class Gather:
    def __init__(self, index, own, slot, half, send, recv, here):
        z, s, y = here
        flip = lax.rem(s + 2, 4)
        other = s + 1 - 2 * lax.rem(s, 2)
        other_flip = lax.rem(other + 2, 4)
        self.near = [(z, flip, y), (z, s, 1 - y), (z, other, y)]
        self.mine, self.from_x, self.from_y, self.from_d = (s, y), (flip, y), (s, 1 - y), (flip, 1 - y)
        self.pair = [(other, y), (other_flip, y), (other, 1 - y), (other_flip, 1 - y)]
        self.index, self.own, self.slot, self.half = index, own, slot, half
        self.send, self.recv = send, recv

    def copy(self, step, src, dst, to):
        return pltpu.make_async_remote_copy(
            src_ref=src,
            dst_ref=dst,
            send_sem=self.send.at[self.index, step],
            recv_sem=self.recv.at[self.index, step],
            device_id=self.near[to],
            device_id_type=MESH,
        )

    def sends(self):
        mine, slot, half = self.slot(self.mine), self.slot, self.half
        return [
            (0, self.own, mine, 0),
            (1, self.own, mine, 1),
            (2, self.own, mine, 2),
            (3, half(self.from_x, 0), half(self.from_x, 0), 1),
            (4, half(self.from_y, 1), half(self.from_y, 1), 0),
            (5, slot(self.from_x), slot(self.from_x), 2),
            (6, slot(self.from_y), slot(self.from_y), 2),
            (7, slot(self.from_d), slot(self.from_d), 2),
        ]

    def begin(self, steps):
        for entry in self.sends():
            if entry[0] in steps:
                self.copy(*entry).start()

    def arrive(self, step):
        where = {
            0: lambda: self.slot(self.from_x),
            1: lambda: self.slot(self.from_y),
            2: lambda: self.slot(self.pair[0]),
            3: lambda: self.half(self.from_d, 0),
            4: lambda: self.half(self.from_d, 1),
            5: lambda: self.slot(self.pair[1]),
            6: lambda: self.slot(self.pair[2]),
            7: lambda: self.slot(self.pair[3]),
        }[step]()
        self.copy(step, where, where, 0).wait_recv()

    def start(self):
        self.begin((0, 1, 2))

    def relay(self):
        self.arrive(0)
        self.begin((3, 5))
        self.arrive(1)
        self.begin((4, 6))

    def relay_far(self):
        self.arrive(3)
        self.arrive(4)
        self.begin((7,))

    def finish(self):
        for step in (2, 5, 6, 7):
            self.arrive(step)

    def drain(self):
        for entry in self.sends():
            self.copy(*entry).wait_send()


def fused_kernel(
    dims, factor,
    g_ref, in_ref, act_ref, w1_hbm, w2_hbm,
    ig_ref, parts,
    acts, deltas, cols, full, edge_s, edge_r, pack_s, pack_r, weight, shifted,
    facc, cacc, near, dl, dpos, zacc, igt, term_s, term_r,
    ag_s, ag_r, c1_s, c1_r, c1_l, c2_s, c2_r, g_s, g_r, h_s, h_r, t_s, t_r, w_sem,
):
    nch, nsx, nsy, rows, lx, ly, nz = dims
    lane = ly * nz
    nk = nsx * nsy
    piece = rows * nch // nk
    sub = piece // 2
    npos = lx * lane
    wide = nsy * lane
    z, s, y = lax.axis_index("ch"), lax.axis_index("sx"), lax.axis_index("sy")
    here = (z, s, y)
    mine = s * nsy + y
    parity = lax.rem(z, 2)
    core = lax.rem(s, 2)
    turn = z // 2

    barrier = pltpu.get_barrier_semaphore()
    for step in range(1, nk):
        k = lax.rem(mine + step, nk)
        pl.semaphore_signal(
            barrier, inc=1, device_id=(z, k // nsy, lax.rem(k, nsy)), device_id_type=MESH
        )
    for step in range(1, nch):
        pl.semaphore_signal(
            barrier, inc=1, device_id=(lax.rem(z + step, nch), s, y), device_id_type=MESH
        )
    pl.semaphore_wait(barrier, nk - 1 + nch - 1)

    load_two = pltpu.make_async_copy(w2_hbm, weight, w_sem.at[0])
    load_two.start()
    load_one = pltpu.make_async_copy(w1_hbm, weight, w_sem.at[1])

    def block_copy(op, ref, q):
        dst_s, dst_y = 2 * (q // 2) + parity, q % 2
        src = ref.at[:, pl.ds(q * sub, sub)]
        dst = cols.at[op, turn, mine]
        remote = pltpu.make_async_remote_copy(
            src_ref=src, dst_ref=dst, send_sem=c1_s.at[op, q], recv_sem=c1_r.at[op, mine],
            device_id=(z, dst_s, dst_y), device_id_type=MESH,
        )
        local = pltpu.make_async_copy(src, dst, c1_l.at[op])
        same = jnp.logical_and(dst_s == s, dst_y == y)
        return same, local, remote

    def blocks_start(op, ref):
        for q in range(nk // 2):
            same, local, remote = block_copy(op, ref, q)

            @pl.when(same)
            def _():
                local.start()

            @pl.when(jnp.logical_not(same))
            def _():
                remote.start()

    def blocks_wait(op, ref):
        @pl.when(parity == core)
        def _():
            for step in range(1, nk):
                k = lax.rem(mine + step, nk)
                dst = cols.at[op, turn, k]
                pltpu.make_async_remote_copy(
                    src_ref=dst, dst_ref=dst, send_sem=c1_s.at[op, 0], recv_sem=c1_r.at[op, k],
                    device_id=here, device_id_type=MESH,
                ).wait_recv()
        for q in range(nk // 2):
            same, local, remote = block_copy(op, ref, q)

            @pl.when(same)
            def _():
                local.wait()

    def blocks_drain(op, ref):
        for q in range(nk // 2):
            same, local, remote = block_copy(op, ref, q)

            @pl.when(jnp.logical_not(same))
            def _():
                remote.wait_send()

    def spread_copy(op, step):
        block = cols.at[op, turn]
        return pltpu.make_async_remote_copy(
            src_ref=block, dst_ref=block, send_sem=c2_s.at[op, step - 1], recv_sem=c2_r.at[op, turn],
            device_id=(lax.rem(z + step, nch), s, y), device_id_type=MESH,
        )

    def spread_start(op):
        @pl.when(parity == core)
        def _():
            for step in range(1, nch):
                spread_copy(op, step).start()

    def spread_wait(op):
        for t in range(2):
            @pl.when(core + 2 * t != z)
            def _():
                block = cols.at[op, t]
                pltpu.make_async_remote_copy(
                    src_ref=block, dst_ref=block, send_sem=c2_s.at[op, 0], recv_sem=c2_r.at[op, t],
                    device_id=here, device_id_type=MESH,
                ).wait_recv()

    def spread_drain(op):
        @pl.when(parity == core)
        def _():
            for step in range(1, nch):
                spread_copy(op, step).wait_send()

    def full_copy(step):
        return pltpu.make_async_remote_copy(
            src_ref=g_ref, dst_ref=full.at[z], send_sem=g_s.at[step - 1], recv_sem=g_r.at[z],
            device_id=(lax.rem(z + step, nch), s, y), device_id_type=MESH,
        )

    def whole(ref):
        slot = lambda k: ref.at[pl.ds(lx * k[0], lx), k[1]]
        half = lambda k, i: ref.at[pl.ds(lx * k[0] + i * (lx // 2), lx // 2), k[1]]
        return slot, half

    act_gather = Gather(0, act_ref, *whole(acts), ag_s, ag_r, here)
    delta_gather = Gather(1, dl, *whole(deltas), ag_s, ag_r, here)
    size = parts.shape[3]
    cut = size // 2 // 16 * 16

    def piece_gather(which, n):
        slot = lambda k: parts.at[which, n, k[0] * nsy + k[1]]
        half = lambda k, i: parts.at[
            which, n, k[0] * nsy + k[1], pl.ds(0, cut) if i == 0 else pl.ds(cut, size - cut)
        ]
        return Gather(2 + 9 * which + n, slot((s, y)), slot, half, ag_s, ag_r, here)

    def clear():
        for b in range(3):
            for p in (0, nsx * lx + 1):
                shifted[b, p] = jnp.zeros(shifted.shape[2:], BF16)
        facc[...] = jnp.zeros(facc.shape, F32)
        for b in range(3):
            for x in range(lx + 2):
                cacc[b, x] = jnp.zeros(cacc.shape[2:], F32)
        zacc[...] = jnp.zeros(zacc.shape, F32)
        acts[pl.ds(lx * s, lx), y] = act_ref[...]
        full[z] = g_ref[...]

    def start_full(beside):
        for step in range(1, nch):
            next_to = {1: z < nch - 1, nch - 1: z > 0}.get(step, z < 0)

            @pl.when(next_to if beside else jnp.logical_not(next_to))
            def _():
                full_copy(step).start()

    def shift_columns(op, b):
        @pl.loop(0, nsx * lx)
        def _(p):
            owner, inner = p // lx, lax.rem(p, lx)
            tiles = [
                jnp.concatenate([cols[op, t, owner * nsy + j, inner] for t in range(2)], axis=0)
                for j in range(nsy)
            ]
            plane = jnp.concatenate(tiles, axis=1).astype(F32)
            where = lanes((piece, wide))
            row, depth = where // nz, lax.rem(where, nz)
            for c in range(3):
                move = (nz * (b - 1) + c - 1) % wide
                value = pltpu.roll(plane, move, 1) if move else plane
                keep = where >= 0
                if b == 0:
                    keep = jnp.logical_and(keep, row < nsy * ly - 1)
                if b == 2:
                    keep = jnp.logical_and(keep, row > 0)
                if c == 0:
                    keep = jnp.logical_and(keep, depth < nz - 1)
                if c == 2:
                    keep = jnp.logical_and(keep, depth > 0)
                value = jnp.where(keep, value, 0.0).astype(BF16)
                for j in range(nsy):
                    shifted[b, p + 1, j, pl.ds(c * piece, piece)] = value[:, j * lane : (j + 1) * lane]

    def filter_pieces(which, left, b):
        @pl.loop(0, 3)
        def _(a):
            facc[:, :rows] = jnp.zeros((facc.shape[0], rows), F32)

            @pl.loop(0, nsx)
            def _(o):
                cells = shifted[b, pl.ds(2 - a + lx * o, lx)]
                other = left[pl.ds(lx * o, lx)]
                cells = jnp.concatenate([cells[i, j] for i in range(lx) for j in range(nsy)], axis=1)
                other = jnp.concatenate([other[i, j] for i in range(lx) for j in range(nsy)], axis=1)
                facc[:, :rows] += dot_lanes(cells, other)

            group = 3 * piece
            n = 3 * a + b
            parts[which, n, mine, pl.ds(0, group)] = (facc[:, :lane] * factor).astype(BF16)
            low = facc[: group // 2, lane : 2 * lane] * factor
            high = facc[group // 2 :, lane : 2 * lane] * factor
            both = jnp.where(lanes(low.shape) < rows - lane, low, swap_halves(high))
            parts[which, n, mine, pl.ds(group, group // 2)] = both.astype(BF16)
            piece_gather(which, n).start()

    def relay_pieces(which, b):
        @pl.loop(0, 3)
        def _(a):
            piece_gather(which, 3 * a + b).relay()

    def far_pieces(which, b):
        @pl.loop(0, 3)
        def _(a):
            piece_gather(which, 3 * a + b).relay_far()

    def finish_pieces(which, first, last):
        @pl.loop(first, last)
        def _(n):
            piece_gather(which, n).finish()

    low_half = lanes((rows, lane)) < nz

    left_dev = (z, lax.rem(s + nsx - 1, nsx), y)
    right_dev = (z, lax.rem(s + 1, nsx), y)

    def halo(i, src, dst, dev):
        return pltpu.make_async_remote_copy(
            src_ref=src, dst_ref=dst, send_sem=h_s.at[i], recv_sem=h_r.at[i],
            device_id=dev, device_id_type=MESH,
        )

    to_y = halo(0, pack_s, pack_r, (z, s, 1 - y))
    to_left = halo(1, edge_s.at[0], edge_r.at[1], left_dev)
    to_right = halo(2, edge_s.at[1], edge_r.at[0], right_dev)
    has_left, has_right = s > 0, s < nsx - 1

    def term_copy(step):
        to = lax.rem(z + step, nch)
        return pltpu.make_async_remote_copy(
            src_ref=term_s.at[to], dst_ref=term_r.at[z], send_sem=t_s.at[step - 1],
            recv_sem=t_r.at[z], device_id=(to, s, y), device_id_type=MESH,
        )

    def wait_full():
        for step in range(1, nch):
            k = lax.rem(z + step, nch)
            pltpu.make_async_remote_copy(
                src_ref=full.at[k], dst_ref=full.at[k], send_sem=g_s.at[0], recv_sem=g_r.at[k],
                device_id=here, device_id_type=MESH,
            ).wait_recv()

    def act_grad():
        load_two.wait()

        @pl.loop(0, 9)
        def _(ab):
            a, b = ab // 3, lax.rem(ab, 3)
            left = weight[pl.ds(3 * ab, 3)].reshape(3 * rows, nch * rows)
            right = jnp.concatenate(
                [jnp.concatenate([full[k, x] for x in range(lx)], axis=1) for k in range(nch)], axis=0
            )
            value = jnp.dot(left, right, preferred_element_type=F32)
            for x in range(lx):
                cacc[b, a + x] += value[:, x * lane : (x + 1) * lane]

        load_one.start()

    def fold_halo():
        depth = lax.rem(lanes((rows, lane)), nz)
        low = None
        for x in range(lx + 2):
            sums = []
            for b in range(3):
                total = cacc[b, x, pl.ds(rows, rows)]
                back = pltpu.roll(cacc[b, x, pl.ds(0, rows)], lane - 1, 1)
                ahead = pltpu.roll(cacc[b, x, pl.ds(2 * rows, rows)], 1, 1)
                total += jnp.where(depth < nz - 1, back, 0.0)
                total += jnp.where(depth > 0, ahead, 0.0)
                sums.append(total)
            up, down = swap_halves(sums[0]), swap_halves(sums[2])
            near[x] = sums[1] + jnp.where(low_half, up, down)
            if x % 2 == 0:
                low = jnp.where(y == 0, down, sums[0])
            else:
                high = jnp.where(y == 0, sums[2], up)
                pack_s[x // 2] = jnp.where(low_half, low, high).astype(BF16)
        to_y.start()

    def fold_edges():
        to_y.wait_recv()
        for x in range(lx + 2):
            value = pack_r[x // 2].astype(F32)
            turned = swap_halves(value)
            to_high, to_low = (turned, value) if x % 2 == 0 else (value, turned)
            high = jnp.where(low_half, 0.0, to_high)
            low = jnp.where(low_half, to_low, 0.0)
            near[x] += jnp.where(y == 0, high, low)
        edge_s[0] = near[0].astype(BF16)
        edge_s[1] = near[lx + 1].astype(BF16)

        @pl.when(has_left)
        def _():
            to_left.start()

        @pl.when(has_right)
        def _():
            to_right.start()

    def make_delta():
        @pl.when(has_right)
        def _():
            to_left.wait_recv()
            near[lx] += edge_r[1].astype(F32)

        @pl.when(has_left)
        def _():
            to_right.wait_recv()
            near[1] += edge_r[0].astype(F32)

        for x in range(lx):
            total = jnp.where(act_ref[x].astype(F32) > 0.0, near[x + 1], 0.0).astype(BF16)
            dl[x] = total
            deltas[lx * s + x, y] = total
        delta_gather.start()

    def place_delta():
        for x in range(lx + 2):
            place = lx * s + x - 1
            inside = jnp.logical_and(place >= 0, place < nsx * lx)
            place = jnp.clip(place, 0, nsx * lx - 1)
            own = deltas[place, y].astype(F32).T
            beside = deltas[place, 1 - y].astype(F32).T
            own = jnp.where(inside, own, 0.0).astype(BF16)
            beside = jnp.where(inside, jnp.where(y == 0, beside[:nz], beside[lane - nz :]), 0.0)
            dpos[x, 0] = jnp.where(y == 0, 0.0, beside).astype(BF16)
            for j in range(ly):
                dpos[x, 1 + j] = own[j * nz : (j + 1) * nz]
            dpos[x, ly + 1] = jnp.where(y == 0, beside, 0.0).astype(BF16)

    def input_terms():
        load_one.wait()

        @pl.loop(0, 9)
        def _(ab):
            a, b = ab // 3, lax.rem(ab, 3)
            left = dpos[pl.ds(2 - a, lx), pl.ds(2 - b, ly)].reshape(npos, rows)
            for c in range(3):
                zacc[c] += jnp.dot(left, weight[3 * ab + c], preferred_element_type=F32)

    def pack_terms():
        for i in range(npos // nz):
            span = slice(i * nz, (i + 1) * nz)
            total = zacc[1, span]
            at = lax.broadcasted_iota(jnp.int32, total.shape, 0)
            total += jnp.where(at < nz - 1, pltpu.roll(zacc[0, span], nz - 1, 0), 0.0)
            total += jnp.where(at > 0, pltpu.roll(zacc[2, span], 1, 0), 0.0)
            igt[span] = total.astype(BF16)

        for k in range(nch):
            shape = (rows, nch * rows)
            pick = lanes(shape) == lax.broadcasted_iota(jnp.int32, shape, 0) + k * rows
            value = dot_lanes(pick.astype(BF16), igt[...]).astype(BF16)
            for x in range(lx):
                term_s[k, x] = value[:, x * lane : (x + 1) * lane]

    def send_terms():
        for step in range(1, nch):
            term_copy(step).start()

    def sum_terms():
        total = term_s[z].astype(F32)
        for step in range(1, nch):
            k = lax.rem(z + step, nch)
            pltpu.make_async_remote_copy(
                src_ref=term_r.at[k], dst_ref=term_r.at[k], send_sem=t_s.at[0], recv_sem=t_r.at[k],
                device_id=here, device_id_type=MESH,
            ).wait_recv()
            total += term_r[k].astype(F32)
        ig_ref[...] = total.astype(BF16)

    blocks_start(0, g_ref)
    act_gather.start()
    start_full(True)
    blocks_start(1, in_ref)
    blocks_wait(0, g_ref)
    spread_start(0)
    clear()
    act_gather.relay()
    act_gather.relay_far()
    act_gather.finish()
    spread_wait(0)
    start_full(False)
    shift_columns(0, 1)
    filter_pieces(0, acts, 1)
    shift_columns(0, 2)
    filter_pieces(0, acts, 2)
    relay_pieces(0, 1)
    shift_columns(0, 0)
    blocks_wait(1, in_ref)
    wait_full()
    spread_start(1)
    act_grad()
    fold_halo()
    relay_pieces(0, 2)
    fold_edges()
    make_delta()
    filter_pieces(0, acts, 0)
    delta_gather.relay()
    spread_wait(1)
    shift_columns(1, 1)
    delta_gather.relay_far()
    relay_pieces(0, 0)
    shift_columns(1, 2)
    delta_gather.finish()
    filter_pieces(1, deltas, 1)
    filter_pieces(1, deltas, 2)
    shift_columns(1, 0)
    for b in (1, 2, 0):
        far_pieces(0, b)
    relay_pieces(1, 1)
    place_delta()
    input_terms()
    pack_terms()
    send_terms()
    finish_pieces(0, 0, 9)
    filter_pieces(1, deltas, 0)
    relay_pieces(1, 2)
    relay_pieces(1, 0)
    for b in range(3):
        far_pieces(1, (b + 1) % 3)
    finish_pieces(1, 0, 9)
    sum_terms()

    for op, ref in ((0, g_ref), (1, in_ref)):
        blocks_drain(op, ref)
        spread_drain(op)
    for step in range(1, nch):
        full_copy(step).wait_send()
        term_copy(step).wait_send()
    to_y.wait_send()

    @pl.when(has_left)
    def _():
        to_left.wait_send()

    @pl.when(has_right)
    def _():
        to_right.wait_send()

    act_gather.drain()
    delta_gather.drain()
    for which in range(2):
        @pl.loop(0, 9)
        def _(n):
            piece_gather(which, n).drain()


def join_kernel(dims, parts, out_two, out_one):
    nch, nsx, nsy, rows, lx, ly, nz = dims
    lane = ly * nz
    nk = nsx * nsy
    piece = rows * nch // nk
    sub = piece // 2
    group = 3 * piece
    rest = rows - lane
    shape = (lane, lane)
    same = (lanes(shape) == lax.broadcasted_iota(jnp.int32, shape, 0)).astype(BF16)
    shape = (rest, lane)
    down = lax.broadcasted_iota(jnp.int32, shape, 0)
    picks = [(lanes(shape) == down + i * rest).astype(BF16) for i in range(2)]
    n = pl.program_id(0)
    for which, out in ((0, out_two), (1, out_one)):
        for c in range(3):
            to = 2 - c if which else c
            main, tail = [], []
            for k in range(nch):
                for q in range(nk // 2):
                    slot = (2 * (q // 2) + k % 2) * nsy + q % 2
                    row = c * piece + (k // 2) * sub
                    main.append(parts[which, n, slot, pl.ds(row, sub)])
                    row = group + (row if row < group // 2 else row - group // 2)
                    tail.append(parts[which, n, slot, pl.ds(row, sub)])
            half = len(main) // 2
            for i in range(2):
                span = slice(i * half * sub, (i + 1) * half * sub)
                part = jnp.concatenate(main[i * half : (i + 1) * half], axis=0)
                out[to, :lane, span] = dot_lanes(same, part)
                part = jnp.concatenate(tail[i * half : (i + 1) * half], axis=0)
                upper = c * piece + i * sub >= group // 2
                out[to, lane:, span] = dot_lanes(picks[1 if upper else 0], part)


def tiles(array):
    rows, lx, ly, nz = array.shape
    return array.reshape(rows, lx, ly * nz).transpose(1, 0, 2)


def fused_shards(inputs, pre_act, out_grad, weight_one, weight_two):
    rows, lx, ly, nz = pre_act.shape
    nch, nsx, nsy = (lax.axis_size(axis) for axis in ("ch", "sx", "sy"))
    dims = (nch, nsx, nsy, rows, lx, ly, nz)
    lane = ly * nz
    nk = nsx * nsy
    channels = nch * rows
    piece = channels // nk
    npos = lx * lane
    factor = 1.0 / math.sqrt(npos * nk)
    size = 3 * piece * rows // lane
    planes = nsx * lx
    tile = (lx, rows, lane)
    vm = lambda *shape: pltpu.VMEM(shape, BF16)
    dma = lambda *shape: pltpu.SemaphoreType.DMA(shape)
    active = jnp.maximum(pre_act, jnp.zeros((), pre_act.dtype))
    grad, pieces = pl.pallas_call(
        functools.partial(fused_kernel, dims, factor),
        out_shape=(
            jax.ShapeDtypeStruct(tile, BF16),
            pltpu.VMEM((2, 9, nk, size, lane), BF16),
        ),
        in_specs=[IN_VMEM] * 3 + [ANY] * 2,
        out_specs=(IN_VMEM, IN_VMEM),
        scratch_shapes=[
            vm(planes, nsy, rows, lane),
            vm(planes, nsy, rows, lane),
            vm(2, 2, nk, lx, piece // 2, lane),
            vm(nch, lx, rows, lane),
            vm(2, rows, lane),
            vm(2, rows, lane),
            vm(lx // 2 + 1, rows, lane),
            vm(lx // 2 + 1, rows, lane),
            vm(27, rows, channels),
            vm(3, planes + 2, nsy, 3 * piece, lane),
            pltpu.VMEM((3 * piece, 2 * lane), F32),
            pltpu.VMEM((3, lx + 2, 3 * rows, lane), F32),
            pltpu.VMEM((lx + 2, rows, lane), F32),
            vm(lx, rows, lane),
            vm(lx + 2, ly + 2, nz, rows),
            pltpu.VMEM((3, npos, channels), F32),
            vm(npos, channels),
            vm(nch, lx, rows, lane),
            vm(nch, lx, rows, lane),
            dma(20, 8), dma(20, 8), dma(2, nk // 2), dma(2, nk), dma(2),
            dma(2, nch - 1), dma(2, 2), dma(nch - 1), dma(nch),
            dma(3), dma(3), dma(nch - 1), dma(nch), dma(2),
        ],
        compiler_params=pltpu.CompilerParams(
            collective_id=0, has_side_effects=True, vmem_limit_bytes=42 * 1024 * 1024
        ),
    )(tiles(out_grad), tiles(inputs), tiles(active), weight_one, weight_two)
    two, one = pl.pallas_call(
        functools.partial(join_kernel, dims),
        grid=(9,),
        out_shape=(jax.ShapeDtypeStruct((27, rows, channels), F32),) * 2,
        in_specs=[IN_VMEM],
        out_specs=(
            pl.BlockSpec((3, rows, channels), lambda n: (n, 0, 0)),
            pl.BlockSpec((3, rows, channels), lambda n: (8 - n, 0, 0)),
        ),
        compiler_params=pltpu.CompilerParams(vmem_limit_bytes=20 * 1024 * 1024),
    )(pieces)
    grad = grad.transpose(1, 0, 2).reshape(rows, lx, ly, nz)
    return grad, one, two


def fits(mesh, rows, lx, ly, nz):
    nch, nsx, nsy = (mesh.shape[axis] for axis in ("ch", "sx", "sy"))
    return (
        (nch, nsx, nsy) == (4, 4, 2)
        and lx % 4 == 0
        and ly == 2
        and ly * nz == 128
        and rows % 64 == 0
        and 128 < rows < 256
    )


def solution(mesh):
    in_specs = (
        P("ch", "sx", "sy", None),
        P("ch", "sx", "sy", None),
        P("ch", "sx", "sy", None),
        P(None, "ch", None),
        P(None, "ch", None),
    )
    out_specs = (P("ch", "sx", "sy", None), P(None, "ch", None), P(None, "ch", None))

    def body(*args):
        return (fused_shards if fits(mesh, *args[1].shape) else shards)(*args)

    return jax.shard_map(body, mesh=mesh, in_specs=in_specs, out_specs=out_specs, check_vma=False)
```

```python
import functools
import math

import jax
import jax.numpy as jnp
from jax import lax
from jax.experimental import pallas as pl
from jax.experimental.pallas import tpu as pltpu
from jax.sharding import PartitionSpec as P


def padded_2(cells, sides, width):
    for axis, dim in sides:
        count = lax.axis_size(axis)
        ends = count - 1
        head = lax.slice_in_dim(cells, 0, width, axis=dim)
        tail = lax.slice_in_dim(cells, cells.shape[dim] - width, cells.shape[dim], axis=dim)
        cells = jnp.concatenate(
            [
                lax.ppermute(tail, axis, [(i, (i + 1) % count) for i in range(ends)]),
                cells,
                lax.ppermute(head, axis, [((i + 1) % count, i) for i in range(ends)]),
            ],
            axis=dim,
        )
    return cells


def window(padded, offset, mirror):
    first = offset // 9
    second = offset // 3 % 3
    third = offset % 3
    if mirror:
        first, second, third = (2 - first, 2 - second, 2 - third)
    size_x = padded.shape[1] - 2
    size_y = padded.shape[2] - 2
    size_z = padded.shape[3] - 2
    part = padded[:, first : first + size_x, second : second + size_y, third : third + size_z]
    return part.reshape(padded.shape[0], size_x * size_y * size_z)


def pad_depth(array):
    return jnp.pad(array, ((0, 0), (0, 0), (0, 0), (1, 1)))


def contract_positions(left, right):
    return lax.dot_general(
        left, right, (((1,), (1,)), ((), ())), preferred_element_type=jnp.float32
    )


def contract_first(left, right):
    return lax.dot_general(
        left, right, (((0,), (0,)), ((), ())), preferred_element_type=jnp.float32
    )


def spread_flat(array):
    padded = jnp.pad(array, ((0, 0), (0, 0), (0, 1), (0, 1)))
    return padded.reshape(padded.shape[0], -1)


def whole_window(blocks, counts):
    count_x, count_y = counts
    channels, size_x, size_y, size_z = blocks.shape[1:]
    grid = blocks.reshape(count_x, count_y, channels, size_x, size_y, size_z)
    grid = grid.transpose(2, 0, 3, 1, 4, 5)
    return grid.reshape(channels, count_x * size_x, count_y * size_y, size_z)


def column_slices(full, counts):
    ranks = counts[0] * counts[1]
    cut = full.reshape(ranks, full.shape[0] // ranks, *full.shape[1:])
    return whole_window(lax.all_to_all(cut, ("sx", "sy"), 0, 0, tiled=True), counts)


def shifts(size_y, size_z):
    row = size_z + 1
    plane = (size_y + 1) * row
    return [
        (a - 1) * plane + (b - 1) * row + c - 1
        for a in range(3)
        for b in range(3)
        for c in range(3)
    ]


def filter_slice(rows, columns, shift_rows):
    steps = shifts(rows.shape[2], rows.shape[3])
    margin = max(steps)
    left = spread_flat(rows)
    size = left.shape[1]
    right = jnp.pad(spread_flat(columns), ((0, 0), (margin, margin)))
    out = []
    for step in steps:
        start = margin - step if shift_rows else margin + step
        part = lax.slice_in_dim(right, start, start + size, axis=1)
        out.append(contract_positions(left, part))
    return jnp.stack(out)


def join_columns(part, factor):
    sent = (part * factor).astype(jnp.bfloat16)
    parts = lax.all_gather(sent, ("sx", "sy"), axis=0)
    return jnp.concatenate([parts[i] for i in range(parts.shape[0])], axis=2).astype(jnp.float32)


def shards(inputs, pre_act, out_grad, weight_one, weight_two):
    shape = pre_act.shape
    positions = shape[1] * shape[2] * shape[3]
    counts = (lax.axis_size("sx"), lax.axis_size("sy"))
    factor = 1.0 / math.sqrt(positions * counts[0] * counts[1])
    full_grad = lax.all_gather(out_grad, "ch", axis=0, tiled=True)
    active = jnp.maximum(pre_act, jnp.zeros((), pre_act.dtype))
    active_all = whole_window(lax.all_gather(active, ("sx", "sy"), axis=0), counts)
    grad_columns = column_slices(full_grad, counts)
    grad_pad = pad_depth(padded_2(full_grad, (("sx", 1), ("sy", 2)), 1))
    filter_two = join_columns(filter_slice(active_all, grad_columns, True), factor)
    act_grad = jnp.zeros((shape[0], positions), jnp.float32)
    for offset in range(27):
        act_grad = act_grad + jnp.dot(
            weight_two[offset], window(grad_pad, offset, True), preferred_element_type=jnp.float32
        )
    delta = jnp.where(pre_act.reshape(shape[0], positions) > 0, act_grad, 0.0).astype(jnp.bfloat16)
    delta = delta.reshape(shape)
    full_in = lax.all_gather(inputs, "ch", axis=0, tiled=True)
    input_columns = column_slices(full_in, counts)
    delta_all = whole_window(lax.all_gather(delta, ("sx", "sy"), axis=0), counts)
    filter_one = join_columns(filter_slice(delta_all, input_columns, False), factor)
    delta_pad = pad_depth(padded_2(delta, (("sx", 1), ("sy", 2)), 1))
    partial_terms = jnp.zeros((weight_one.shape[2], positions), jnp.float32)
    for offset in range(27):
        partial_terms = partial_terms + contract_first(
            weight_one[offset], window(delta_pad, offset, True)
        )
    partial_terms = partial_terms.reshape(weight_one.shape[2], shape[1], shape[2], shape[3])
    input_grad = lax.psum_scatter(partial_terms, "ch", scatter_dimension=0, tiled=True).astype(
        jnp.bfloat16
    )
    return (input_grad, filter_one, filter_two)


F32 = jnp.float32
BF16 = jnp.bfloat16
MESH = pl.DeviceIdType.MESH
ANY = pl.BlockSpec(memory_space=pl.ANY)
IN_VMEM = pl.BlockSpec(memory_space=pltpu.VMEM)


def dot_lanes(left, right):
    return lax.dot_general(left, right, (((1,), (1,)), ((), ())), preferred_element_type=F32)


def lanes(shape):
    return lax.broadcasted_iota(jnp.int32, shape, len(shape) - 1)


def swap_halves(tile):
    return pltpu.roll(tile, tile.shape[-1] // 2, 1)


class Gather:
    def __init__(self, index, own, slot, half, send, recv, here):
        z, s, y = here
        flip = lax.rem(s + 2, 4)
        other = s + 1 - 2 * lax.rem(s, 2)
        other_flip = lax.rem(other + 2, 4)
        self.near = [(z, flip, y), (z, s, 1 - y), (z, other, y)]
        self.mine, self.from_x, self.from_y, self.from_d = (s, y), (flip, y), (s, 1 - y), (flip, 1 - y)
        self.pair = [(other, y), (other_flip, y), (other, 1 - y), (other_flip, 1 - y)]
        self.index, self.own, self.slot, self.half = index, own, slot, half
        self.send, self.recv = send, recv

    def copy(self, step, src, dst, to):
        return pltpu.make_async_remote_copy(
            src_ref=src,
            dst_ref=dst,
            send_sem=self.send.at[self.index, step],
            recv_sem=self.recv.at[self.index, step],
            device_id=self.near[to],
            device_id_type=MESH,
        )

    def sends(self):
        mine, slot, half = self.slot(self.mine), self.slot, self.half
        return [
            (0, self.own, mine, 0),
            (1, self.own, mine, 1),
            (2, self.own, mine, 2),
            (3, half(self.from_x, 0), half(self.from_x, 0), 1),
            (4, half(self.from_y, 1), half(self.from_y, 1), 0),
            (5, slot(self.from_x), slot(self.from_x), 2),
            (6, slot(self.from_y), slot(self.from_y), 2),
            (7, slot(self.from_d), slot(self.from_d), 2),
        ]

    def begin(self, steps):
        for entry in self.sends():
            if entry[0] in steps:
                self.copy(*entry).start()

    def arrive(self, step):
        where = {
            0: lambda: self.slot(self.from_x),
            1: lambda: self.slot(self.from_y),
            2: lambda: self.slot(self.pair[0]),
            3: lambda: self.half(self.from_d, 0),
            4: lambda: self.half(self.from_d, 1),
            5: lambda: self.slot(self.pair[1]),
            6: lambda: self.slot(self.pair[2]),
            7: lambda: self.slot(self.pair[3]),
        }[step]()
        self.copy(step, where, where, 0).wait_recv()

    def start(self):
        self.begin((0, 1, 2))

    def relay(self):
        self.arrive(0)
        self.begin((3, 5))
        self.arrive(1)
        self.begin((4, 6))

    def relay_far(self):
        self.arrive(3)
        self.arrive(4)
        self.begin((7,))

    def finish(self):
        for step in (2, 5, 6, 7):
            self.arrive(step)

    def drain(self):
        for entry in self.sends():
            self.copy(*entry).wait_send()


def fused_kernel(
    dims, factor,
    own_ref, w1_hbm, w2_hbm,
    ig_ref, parts,
    acts, deltas, cols, full, edge_s, edge_r, pack_s, pack_r, weight, shifted,
    facc, cacc, near, dl, dpos, zacc, igt, term_s, term_r,
    ag_s, ag_r, c1_s, c1_r, c1_l, c2_s, c2_r, g_s, g_r, h_s, h_r, t_s, t_r, w_sem,
):
    nch, nsx, nsy, rows, lx, ly, nz = dims
    g_ref, in_ref, act_ref = (own_ref.at[:, pl.ds(i * rows, rows)] for i in range(3))
    lane = ly * nz
    nk = nsx * nsy
    piece = rows * nch // nk
    sub = piece // 2
    npos = lx * lane
    wide = nsy * lane
    z, s, y = lax.axis_index("ch"), lax.axis_index("sx"), lax.axis_index("sy")
    here = (z, s, y)
    mine = s * nsy + y
    parity = lax.rem(z, 2)
    core = lax.rem(s, 2)
    turn = z // 2

    barrier = pltpu.get_barrier_semaphore()
    for step in range(1, nk):
        k = lax.rem(mine + step, nk)
        pl.semaphore_signal(
            barrier, inc=1, device_id=(z, k // nsy, lax.rem(k, nsy)), device_id_type=MESH
        )
    for step in range(1, nch):
        pl.semaphore_signal(
            barrier, inc=1, device_id=(lax.rem(z + step, nch), s, y), device_id_type=MESH
        )
    pl.semaphore_wait(barrier, nk - 1 + nch - 1)

    load_two = pltpu.make_async_copy(w2_hbm, weight, w_sem.at[0])
    load_two.start()
    load_one = pltpu.make_async_copy(w1_hbm, weight, w_sem.at[1])

    def block_copy(op, ref, q):
        dst_s, dst_y = 2 * (q // 2) + parity, q % 2
        src = ref.at[:, pl.ds(q * sub, sub)]
        dst = cols.at[op, turn, mine]
        remote = pltpu.make_async_remote_copy(
            src_ref=src, dst_ref=dst, send_sem=c1_s.at[op, q], recv_sem=c1_r.at[op, mine],
            device_id=(z, dst_s, dst_y), device_id_type=MESH,
        )
        local = pltpu.make_async_copy(src, dst, c1_l.at[op])
        same = jnp.logical_and(dst_s == s, dst_y == y)
        return same, local, remote

    def blocks_start(op, ref):
        for q in range(nk // 2):
            same, local, remote = block_copy(op, ref, q)

            @pl.when(same)
            def _():
                local.start()

            @pl.when(jnp.logical_not(same))
            def _():
                remote.start()

    def blocks_wait(op, ref):
        @pl.when(parity == core)
        def _():
            for step in range(1, nk):
                k = lax.rem(mine + step, nk)
                dst = cols.at[op, turn, k]
                pltpu.make_async_remote_copy(
                    src_ref=dst, dst_ref=dst, send_sem=c1_s.at[op, 0], recv_sem=c1_r.at[op, k],
                    device_id=here, device_id_type=MESH,
                ).wait_recv()
        for q in range(nk // 2):
            same, local, remote = block_copy(op, ref, q)

            @pl.when(same)
            def _():
                local.wait()

    def blocks_drain(op, ref):
        for q in range(nk // 2):
            same, local, remote = block_copy(op, ref, q)

            @pl.when(jnp.logical_not(same))
            def _():
                remote.wait_send()

    def spread_copy(op, step):
        block = cols.at[op, turn]
        return pltpu.make_async_remote_copy(
            src_ref=block, dst_ref=block, send_sem=c2_s.at[op, step - 1], recv_sem=c2_r.at[op, turn],
            device_id=(lax.rem(z + step, nch), s, y), device_id_type=MESH,
        )

    def spread_start(op):
        @pl.when(parity == core)
        def _():
            for step in range(1, nch):
                spread_copy(op, step).start()

    def spread_wait(op, t):
        @pl.when(core + 2 * t != z)
        def _():
            block = cols.at[op, t]
            pltpu.make_async_remote_copy(
                src_ref=block, dst_ref=block, send_sem=c2_s.at[op, 0], recv_sem=c2_r.at[op, t],
                device_id=here, device_id_type=MESH,
            ).wait_recv()

    def spread_drain(op):
        @pl.when(parity == core)
        def _():
            for step in range(1, nch):
                spread_copy(op, step).wait_send()

    def full_pass(hop, to):
        k = z - hop if to else z + hop
        valid = jnp.logical_and(k >= 0, z < nch - 1) if to else jnp.logical_and(k < nch, z > 0)
        k = jnp.clip(k, 0, nch - 1)
        copy = pltpu.make_async_remote_copy(
            src_ref=g_ref if hop == 0 else full.at[k], dst_ref=full.at[k],
            send_sem=g_s.at[hop, to], recv_sem=g_r.at[k],
            device_id=(jnp.clip(z + 2 * to - 1, 0, nch - 1), s, y), device_id_type=MESH,
        )
        return valid, copy

    def start_full(hop):
        for to in range(2):
            valid, copy = full_pass(hop, to)

            @pl.when(valid)
            def _():
                copy.start()

    def drain_full():
        for hop in range(nch - 1):
            for to in range(2):
                valid, copy = full_pass(hop, to)

                @pl.when(valid)
                def _():
                    copy.wait_send()

    def wait_full(hop):
        for k, valid in ((z - hop, z >= hop), (z + hop, z + hop < nch)):
            k = jnp.clip(k, 0, nch - 1)

            @pl.when(valid)
            def _():
                pltpu.make_async_remote_copy(
                    src_ref=full.at[k], dst_ref=full.at[k], send_sem=g_s.at[0, 0],
                    recv_sem=g_r.at[k], device_id=here, device_id_type=MESH,
                ).wait_recv()

    def whole(ref):
        slot = lambda k: ref.at[pl.ds(lx * k[0], lx), k[1]]
        half = lambda k, i: ref.at[pl.ds(lx * k[0] + i * (lx // 2), lx // 2), k[1]]
        return slot, half

    act_gather = Gather(0, act_ref, *whole(acts), ag_s, ag_r, here)
    delta_gather = Gather(1, dl, *whole(deltas), ag_s, ag_r, here)
    size = parts.shape[3]
    cut = size // 2 // 16 * 16

    def piece_gather(which, n):
        slot = lambda k: parts.at[which, n, k[0] * nsy + k[1]]
        half = lambda k, i: parts.at[
            which, n, k[0] * nsy + k[1], pl.ds(0, cut) if i == 0 else pl.ds(cut, size - cut)
        ]
        return Gather(2 + 6 * which + n, slot((s, y)), slot, half, ag_s, ag_r, here)

    def clear():
        for t in range(2):
            for p in (0, nsx * lx + 1):
                shifted[t, p] = jnp.zeros(shifted.shape[2:], BF16)
        facc[...] = jnp.zeros(facc.shape, F32)
        for b in range(3):
            for x in range(lx + 2):
                cacc[b, x] = jnp.zeros(cacc.shape[2:], F32)
        zacc[...] = jnp.zeros(zacc.shape, F32)
        acts[pl.ds(lx * s, lx), y] = act_ref[...]
        full[z] = g_ref[...]

    def shift_columns(op, t):
        @pl.loop(0, nsx * lx)
        def _(p):
            owner, inner = p // lx, lax.rem(p, lx)
            tiles = [cols[op, t, owner * nsy + j, inner] for j in range(nsy)]
            plane = jnp.concatenate(tiles, axis=1).astype(F32)
            where = lanes((sub, wide))
            row, depth = where // nz, lax.rem(where, nz)
            for b in range(3):
                for c in range(3):
                    move = (nz * (b - 1) + c - 1) % wide
                    value = pltpu.roll(plane, move, 1) if move else plane
                    keep = where >= 0
                    if b == 0:
                        keep = jnp.logical_and(keep, row < nsy * ly - 1)
                    if b == 2:
                        keep = jnp.logical_and(keep, row > 0)
                    if c == 0:
                        keep = jnp.logical_and(keep, depth < nz - 1)
                    if c == 2:
                        keep = jnp.logical_and(keep, depth > 0)
                    value = jnp.where(keep, value, 0.0).astype(BF16)
                    for j in range(nsy):
                        shifted[t, p + 1, j, pl.ds((3 * b + c) * sub, sub)] = value[
                            :, j * lane : (j + 1) * lane
                        ]

    def filter_pieces(which, left, t):
        @pl.loop(0, 3)
        def _(a):
            facc[:, :rows] = jnp.zeros((facc.shape[0], rows), F32)

            @pl.loop(0, nsx)
            def _(o):
                cells = shifted[t, pl.ds(2 - a + lx * o, lx)]
                other = left[pl.ds(lx * o, lx)]
                cells = jnp.concatenate([cells[i, j] for i in range(lx) for j in range(nsy)], axis=1)
                other = jnp.concatenate([other[i, j] for i in range(lx) for j in range(nsy)], axis=1)
                facc[:, :rows] += dot_lanes(cells, other)

            group = 9 * sub
            n = 3 * t + a
            parts[which, n, mine, pl.ds(0, group)] = (facc[:, :lane] * factor).astype(BF16)
            for low, high, size_of, to in ((0, 4 * sub, 4 * sub, 0), (8 * sub, 17 * sub // 2, sub // 2, 4 * sub)):
                first = facc[pl.ds(low, size_of), lane : 2 * lane] * factor
                second = facc[pl.ds(high, size_of), lane : 2 * lane] * factor
                both = jnp.where(lanes(first.shape) < rows - lane, first, swap_halves(second))
                parts[which, n, mine, pl.ds(group + to, size_of)] = both.astype(BF16)
            piece_gather(which, n).start()

    def relay_pieces(which, t):
        @pl.loop(0, 3)
        def _(a):
            piece_gather(which, 3 * t + a).relay()

    def far_pieces(which, t):
        @pl.loop(0, 3)
        def _(a):
            piece_gather(which, 3 * t + a).relay_far()

    def finish_pieces(which):
        @pl.loop(0, 6)
        def _(n):
            piece_gather(which, n).finish()

    low_half = lanes((rows, lane)) < nz

    left_dev = (z, lax.rem(s + nsx - 1, nsx), y)
    right_dev = (z, lax.rem(s + 1, nsx), y)

    def halo(i, src, dst, dev):
        return pltpu.make_async_remote_copy(
            src_ref=src, dst_ref=dst, send_sem=h_s.at[i], recv_sem=h_r.at[i],
            device_id=dev, device_id_type=MESH,
        )

    to_y = halo(0, pack_s, pack_r, (z, s, 1 - y))
    to_left = halo(1, edge_s.at[0], edge_r.at[1], left_dev)
    to_right = halo(2, edge_s.at[1], edge_r.at[0], right_dev)
    has_left, has_right = s > 0, s < nsx - 1

    def term_copy(step):
        to = lax.rem(z + step, nch)
        return pltpu.make_async_remote_copy(
            src_ref=term_s.at[to], dst_ref=term_r.at[z], send_sem=t_s.at[step - 1],
            recv_sem=t_r.at[z], device_id=(to, s, y), device_id_type=MESH,
        )

    def act_grad():
        load_two.wait()

        @pl.loop(0, 9)
        def _(ab):
            a, b = ab // 3, lax.rem(ab, 3)
            left = weight[pl.ds(3 * ab, 3)].reshape(3 * rows, nch * rows)
            right = jnp.concatenate(
                [jnp.concatenate([full[k, x] for x in range(lx)], axis=1) for k in range(nch)], axis=0
            )
            value = jnp.dot(left, right, preferred_element_type=F32)
            for x in range(lx):
                cacc[b, a + x] += value[:, x * lane : (x + 1) * lane]

        load_one.start()

    def fold_halo():
        depth = lax.rem(lanes((rows, lane)), nz)
        low = None
        for x in range(lx + 2):
            sums = []
            for b in range(3):
                total = cacc[b, x, pl.ds(rows, rows)]
                back = pltpu.roll(cacc[b, x, pl.ds(0, rows)], lane - 1, 1)
                ahead = pltpu.roll(cacc[b, x, pl.ds(2 * rows, rows)], 1, 1)
                total += jnp.where(depth < nz - 1, back, 0.0)
                total += jnp.where(depth > 0, ahead, 0.0)
                sums.append(total)
            up, down = swap_halves(sums[0]), swap_halves(sums[2])
            near[x] = sums[1] + jnp.where(low_half, up, down)
            if x % 2 == 0:
                low = jnp.where(y == 0, down, sums[0])
            else:
                high = jnp.where(y == 0, sums[2], up)
                pack_s[x // 2] = jnp.where(low_half, low, high).astype(BF16)
        to_y.start()

    def fold_edges():
        to_y.wait_recv()
        for x in range(lx + 2):
            value = pack_r[x // 2].astype(F32)
            turned = swap_halves(value)
            to_high, to_low = (turned, value) if x % 2 == 0 else (value, turned)
            high = jnp.where(low_half, 0.0, to_high)
            low = jnp.where(low_half, to_low, 0.0)
            near[x] += jnp.where(y == 0, high, low)
        edge_s[0] = near[0].astype(BF16)
        edge_s[1] = near[lx + 1].astype(BF16)

        @pl.when(has_left)
        def _():
            to_left.start()

        @pl.when(has_right)
        def _():
            to_right.start()

    def make_delta():
        @pl.when(has_right)
        def _():
            to_left.wait_recv()
            near[lx] += edge_r[1].astype(F32)

        @pl.when(has_left)
        def _():
            to_right.wait_recv()
            near[1] += edge_r[0].astype(F32)

        for x in range(lx):
            total = jnp.where(act_ref[x].astype(F32) > 0.0, near[x + 1], 0.0).astype(BF16)
            dl[x] = total
            deltas[lx * s + x, y] = total
        delta_gather.start()

    def place_delta():
        for x in range(lx + 2):
            place = lx * s + x - 1
            inside = jnp.logical_and(place >= 0, place < nsx * lx)
            place = jnp.clip(place, 0, nsx * lx - 1)
            own = deltas[place, y].astype(F32).T
            beside = deltas[place, 1 - y].astype(F32).T
            own = jnp.where(inside, own, 0.0).astype(BF16)
            beside = jnp.where(inside, jnp.where(y == 0, beside[:nz], beside[lane - nz :]), 0.0)
            dpos[x, 0] = jnp.where(y == 0, 0.0, beside).astype(BF16)
            for j in range(ly):
                dpos[x, 1 + j] = own[j * nz : (j + 1) * nz]
            dpos[x, ly + 1] = jnp.where(y == 0, beside, 0.0).astype(BF16)

    def input_terms(first, last):
        @pl.loop(first, last)
        def _(ab):
            a, b = ab // 3, lax.rem(ab, 3)
            left = dpos[pl.ds(2 - a, lx), pl.ds(2 - b, ly)].reshape(npos, rows)
            for c in range(3):
                zacc[c] += jnp.dot(left, weight[3 * ab + c], preferred_element_type=F32)

    def pack_terms():
        for i in range(npos // nz):
            span = slice(i * nz, (i + 1) * nz)
            total = zacc[1, span]
            at = lax.broadcasted_iota(jnp.int32, total.shape, 0)
            total += jnp.where(at < nz - 1, pltpu.roll(zacc[0, span], nz - 1, 0), 0.0)
            total += jnp.where(at > 0, pltpu.roll(zacc[2, span], 1, 0), 0.0)
            igt[span] = total.astype(BF16)

        for k in range(nch):
            shape = (rows, nch * rows)
            pick = lanes(shape) == lax.broadcasted_iota(jnp.int32, shape, 0) + k * rows
            value = dot_lanes(pick.astype(BF16), igt[...]).astype(BF16)
            for x in range(lx):
                term_s[k, x] = value[:, x * lane : (x + 1) * lane]

    def send_terms():
        for step in range(1, nch):
            term_copy(step).start()

    def sum_terms():
        total = term_s[z].astype(F32)
        for step in range(1, nch):
            k = lax.rem(z + step, nch)
            pltpu.make_async_remote_copy(
                src_ref=term_r.at[k], dst_ref=term_r.at[k], send_sem=t_s.at[0], recv_sem=t_r.at[k],
                device_id=here, device_id_type=MESH,
            ).wait_recv()
            total += term_r[k].astype(F32)
        ig_ref[...] = total.astype(BF16)

    def drain_columns():
        for op, ref in ((0, g_ref), (1, in_ref)):
            blocks_drain(op, ref)
            spread_drain(op)
        drain_full()

    def drain_halo():
        for step in range(1, nch):
            term_copy(step).wait_send()
        to_y.wait_send()

        @pl.when(has_left)
        def _():
            to_left.wait_send()

        @pl.when(has_right)
        def _():
            to_right.wait_send()

        act_gather.drain()
        delta_gather.drain()

    def drain_pieces(which):
        @pl.loop(0, 6)
        def _(n):
            piece_gather(which, n).drain()

    blocks_start(0, g_ref)
    act_gather.start()
    start_full(0)
    blocks_wait(0, g_ref)
    spread_start(0)
    clear()
    act_gather.relay()

    @pl.when(parity == core)
    def _():
        shift_columns(0, turn)

    act_gather.relay_far()
    act_gather.finish()

    @pl.when(parity != core)
    def _():
        spread_wait(0, turn)
        shift_columns(0, turn)

    filter_pieces(0, acts, turn)
    spread_wait(0, 1 - turn)
    wait_full(1)
    start_full(1)
    blocks_start(1, in_ref)
    shift_columns(0, 1 - turn)
    relay_pieces(0, turn)
    wait_full(2)
    start_full(2)
    filter_pieces(0, acts, 1 - turn)
    blocks_wait(1, in_ref)
    wait_full(3)
    spread_start(1)
    act_grad()
    fold_halo()
    fold_edges()
    make_delta()
    relay_pieces(0, 1 - turn)
    far_pieces(0, turn)
    delta_gather.relay()
    spread_wait(1, turn)
    shift_columns(1, turn)
    delta_gather.relay_far()
    spread_wait(1, 1 - turn)
    shift_columns(1, 1 - turn)
    delta_gather.finish()
    filter_pieces(1, deltas, turn)
    far_pieces(0, 1 - turn)
    place_delta()
    load_one.wait()
    input_terms(0, 9)
    pack_terms()
    send_terms()
    relay_pieces(1, turn)
    filter_pieces(1, deltas, 1 - turn)
    finish_pieces(0)
    drain_columns()
    drain_pieces(0)
    relay_pieces(1, 1 - turn)
    far_pieces(1, turn)
    far_pieces(1, 1 - turn)
    sum_terms()
    drain_halo()
    finish_pieces(1)
    drain_pieces(1)


def join_kernel(dims, parts, out_two, out_one):
    nch, nsx, nsy, rows, lx, ly, nz = dims
    lane = ly * nz
    nk = nsx * nsy
    sub = rows * nch // nk // 2
    group = 9 * sub
    rest = rows - lane
    a = pl.program_id(0) // 3
    shape = (lane, lane)
    same = (lanes(shape) == lax.broadcasted_iota(jnp.int32, shape, 0)).astype(BF16)
    shape = (rest, lane)
    down, across = lax.broadcasted_iota(jnp.int32, shape, 0), lanes(shape)
    picks = [(across == down).astype(BF16), (across == down + rest).astype(BF16)]
    shape = (sub, lane)
    own_half = lax.broadcasted_iota(jnp.int32, shape, 0) // (sub // 2) == lanes(shape) // rest

    def gathered(which, load):
        found = []
        for k in range(nch):
            for q in range(nk // 2):
                slot = (2 * (q // 2) + k % 2) * nsy + q % 2
                found.append(load((which, 3 * (k // 2) + a, slot)))
        return jnp.concatenate(found, axis=0)

    def join(b, c, which, out):
        block = 3 * b + c
        out[:lane] = dot_lanes(same, gathered(which, lambda at: parts[(*at, pl.ds(block * sub, sub))]))
        start = group + block % 4 * sub
        if block < 8:
            tail = gathered(which, lambda at: parts[(*at, pl.ds(start, sub))])
            out[lane:] = dot_lanes(picks[block // 4], tail)
        else:
            def load(at):
                half = parts[(*at, pl.ds(group + 4 * sub, sub // 2))].astype(F32)
                both = jnp.concatenate([half, half], axis=0)
                return jnp.where(own_half, both, 0.0).astype(BF16)

            out[lane:] = dot_lanes(picks[0] + picks[1], gathered(which, load))

    for b in range(3):
        @pl.when(lax.rem(pl.program_id(0), 3) == b)
        def _():
            for c in range(3):
                join(b, c, 0, out_two.at[c])
                join(b, c, 1, out_one.at[2 - c])


def tiles(array):
    rows, lx, ly, nz = array.shape
    return array.reshape(rows, lx, ly * nz).transpose(1, 0, 2)


def fused_shards(inputs, pre_act, out_grad, weight_one, weight_two):
    rows, lx, ly, nz = pre_act.shape
    nch, nsx, nsy = (lax.axis_size(axis) for axis in ("ch", "sx", "sy"))
    dims = (nch, nsx, nsy, rows, lx, ly, nz)
    lane = ly * nz
    nk = nsx * nsy
    channels = nch * rows
    piece = channels // nk
    npos = lx * lane
    factor = 1.0 / math.sqrt(npos * nk)
    size = 9 * piece // 2 * rows // lane
    planes = nsx * lx
    tile = (lx, rows, lane)
    vm = lambda *shape: pltpu.VMEM(shape, BF16)
    dma = lambda *shape: pltpu.SemaphoreType.DMA(shape)
    active = jnp.maximum(pre_act, jnp.zeros((), pre_act.dtype))
    own = tiles(jnp.concatenate([out_grad, inputs, active], axis=0))
    grad, pieces = pl.pallas_call(
        functools.partial(fused_kernel, dims, factor),
        out_shape=(
            jax.ShapeDtypeStruct(tile, BF16),
            pltpu.VMEM((2, 6, nk, size, lane), BF16),
        ),
        in_specs=[IN_VMEM] + [ANY] * 2,
        out_specs=(IN_VMEM, IN_VMEM),
        scratch_shapes=[
            vm(planes, nsy, rows, lane),
            vm(planes, nsy, rows, lane),
            vm(2, 2, nk, lx, piece // 2, lane),
            vm(nch, lx, rows, lane),
            vm(2, rows, lane),
            vm(2, rows, lane),
            vm(lx // 2 + 1, rows, lane),
            vm(lx // 2 + 1, rows, lane),
            vm(27, rows, channels),
            vm(2, planes + 2, nsy, 9 * piece // 2, lane),
            pltpu.VMEM((9 * piece // 2, 2 * lane), F32),
            pltpu.VMEM((3, lx + 2, 3 * rows, lane), F32),
            pltpu.VMEM((lx + 2, rows, lane), F32),
            vm(lx, rows, lane),
            vm(lx + 2, ly + 2, nz, rows),
            pltpu.VMEM((3, npos, channels), F32),
            vm(npos, channels),
            vm(nch, lx, rows, lane),
            vm(nch, lx, rows, lane),
            dma(14, 8), dma(14, 8), dma(2, nk // 2), dma(2, nk), dma(2),
            dma(2, nch - 1), dma(2, 2), dma(nch - 1, 2), dma(nch),
            dma(3), dma(3), dma(nch - 1), dma(nch), dma(2),
        ],
        compiler_params=pltpu.CompilerParams(
            collective_id=0, has_side_effects=True, vmem_limit_bytes=42 * 1024 * 1024
        ),
    )(own, weight_one, weight_two)
    two, one = pl.pallas_call(
        functools.partial(join_kernel, dims),
        grid=(9,),
        out_shape=(jax.ShapeDtypeStruct((27, rows, channels), F32),) * 2,
        in_specs=[IN_VMEM],
        out_specs=(
            pl.BlockSpec((3, rows, channels), lambda n: (n, 0, 0)),
            pl.BlockSpec((3, rows, channels), lambda n: (8 - n, 0, 0)),
        ),
        compiler_params=pltpu.CompilerParams(vmem_limit_bytes=20 * 1024 * 1024),
    )(pieces)
    grad = grad.transpose(1, 0, 2).reshape(rows, lx, ly, nz)
    return grad, one, two


def fits(mesh, rows, lx, ly, nz):
    nch, nsx, nsy = (mesh.shape[axis] for axis in ("ch", "sx", "sy"))
    return (
        (nch, nsx, nsy) == (4, 4, 2)
        and lx % 4 == 0
        and ly == 2
        and ly * nz == 128
        and rows % 64 == 0
        and 128 < rows < 256
    )


def solution(mesh):
    in_specs = (
        P("ch", "sx", "sy", None),
        P("ch", "sx", "sy", None),
        P("ch", "sx", "sy", None),
        P(None, "ch", None),
        P(None, "ch", None),
    )
    out_specs = (P("ch", "sx", "sy", None), P(None, "ch", None), P(None, "ch", None))

    def body(*args):
        return (fused_shards if fits(mesh, *args[1].shape) else shards)(*args)

    return jax.shard_map(body, mesh=mesh, in_specs=in_specs, out_specs=out_specs, check_vma=False)
```

```python
import functools
import math

import jax
import jax.numpy as jnp
from jax import lax
from jax.experimental import pallas as pl
from jax.experimental.pallas import tpu as pltpu
from jax.sharding import PartitionSpec as P


def padded_2(cells, sides, width):
    for axis, dim in sides:
        count = lax.axis_size(axis)
        ends = count - 1
        head = lax.slice_in_dim(cells, 0, width, axis=dim)
        tail = lax.slice_in_dim(cells, cells.shape[dim] - width, cells.shape[dim], axis=dim)
        cells = jnp.concatenate(
            [
                lax.ppermute(tail, axis, [(i, (i + 1) % count) for i in range(ends)]),
                cells,
                lax.ppermute(head, axis, [((i + 1) % count, i) for i in range(ends)]),
            ],
            axis=dim,
        )
    return cells


def window(padded, offset, mirror):
    first = offset // 9
    second = offset // 3 % 3
    third = offset % 3
    if mirror:
        first, second, third = (2 - first, 2 - second, 2 - third)
    size_x = padded.shape[1] - 2
    size_y = padded.shape[2] - 2
    size_z = padded.shape[3] - 2
    part = padded[:, first : first + size_x, second : second + size_y, third : third + size_z]
    return part.reshape(padded.shape[0], size_x * size_y * size_z)


def pad_depth(array):
    return jnp.pad(array, ((0, 0), (0, 0), (0, 0), (1, 1)))


def contract_positions(left, right):
    return lax.dot_general(
        left, right, (((1,), (1,)), ((), ())), preferred_element_type=jnp.float32
    )


def contract_first(left, right):
    return lax.dot_general(
        left, right, (((0,), (0,)), ((), ())), preferred_element_type=jnp.float32
    )


def spread_flat(array):
    padded = jnp.pad(array, ((0, 0), (0, 0), (0, 1), (0, 1)))
    return padded.reshape(padded.shape[0], -1)


def whole_window(blocks, counts):
    count_x, count_y = counts
    channels, size_x, size_y, size_z = blocks.shape[1:]
    grid = blocks.reshape(count_x, count_y, channels, size_x, size_y, size_z)
    grid = grid.transpose(2, 0, 3, 1, 4, 5)
    return grid.reshape(channels, count_x * size_x, count_y * size_y, size_z)


def column_slices(full, counts):
    ranks = counts[0] * counts[1]
    cut = full.reshape(ranks, full.shape[0] // ranks, *full.shape[1:])
    return whole_window(lax.all_to_all(cut, ("sx", "sy"), 0, 0, tiled=True), counts)


def shifts(size_y, size_z):
    row = size_z + 1
    plane = (size_y + 1) * row
    return [
        (a - 1) * plane + (b - 1) * row + c - 1
        for a in range(3)
        for b in range(3)
        for c in range(3)
    ]


def filter_slice(rows, columns, shift_rows):
    steps = shifts(rows.shape[2], rows.shape[3])
    margin = max(steps)
    left = spread_flat(rows)
    size = left.shape[1]
    right = jnp.pad(spread_flat(columns), ((0, 0), (margin, margin)))
    out = []
    for step in steps:
        start = margin - step if shift_rows else margin + step
        part = lax.slice_in_dim(right, start, start + size, axis=1)
        out.append(contract_positions(left, part))
    return jnp.stack(out)


def join_columns(part, factor):
    sent = (part * factor).astype(jnp.bfloat16)
    parts = lax.all_gather(sent, ("sx", "sy"), axis=0)
    return jnp.concatenate([parts[i] for i in range(parts.shape[0])], axis=2).astype(jnp.float32)


def shards(inputs, pre_act, out_grad, weight_one, weight_two):
    shape = pre_act.shape
    positions = shape[1] * shape[2] * shape[3]
    counts = (lax.axis_size("sx"), lax.axis_size("sy"))
    factor = 1.0 / math.sqrt(positions * counts[0] * counts[1])
    full_grad = lax.all_gather(out_grad, "ch", axis=0, tiled=True)
    active = jnp.maximum(pre_act, jnp.zeros((), pre_act.dtype))
    active_all = whole_window(lax.all_gather(active, ("sx", "sy"), axis=0), counts)
    grad_columns = column_slices(full_grad, counts)
    grad_pad = pad_depth(padded_2(full_grad, (("sx", 1), ("sy", 2)), 1))
    filter_two = join_columns(filter_slice(active_all, grad_columns, True), factor)
    act_grad = jnp.zeros((shape[0], positions), jnp.float32)
    for offset in range(27):
        act_grad = act_grad + jnp.dot(
            weight_two[offset], window(grad_pad, offset, True), preferred_element_type=jnp.float32
        )
    delta = jnp.where(pre_act.reshape(shape[0], positions) > 0, act_grad, 0.0).astype(jnp.bfloat16)
    delta = delta.reshape(shape)
    full_in = lax.all_gather(inputs, "ch", axis=0, tiled=True)
    input_columns = column_slices(full_in, counts)
    delta_all = whole_window(lax.all_gather(delta, ("sx", "sy"), axis=0), counts)
    filter_one = join_columns(filter_slice(delta_all, input_columns, False), factor)
    delta_pad = pad_depth(padded_2(delta, (("sx", 1), ("sy", 2)), 1))
    partial_terms = jnp.zeros((weight_one.shape[2], positions), jnp.float32)
    for offset in range(27):
        partial_terms = partial_terms + contract_first(
            weight_one[offset], window(delta_pad, offset, True)
        )
    partial_terms = partial_terms.reshape(weight_one.shape[2], shape[1], shape[2], shape[3])
    input_grad = lax.psum_scatter(partial_terms, "ch", scatter_dimension=0, tiled=True).astype(
        jnp.bfloat16
    )
    return (input_grad, filter_one, filter_two)


F32 = jnp.float32
BF16 = jnp.bfloat16
MESH = pl.DeviceIdType.MESH
ANY = pl.BlockSpec(memory_space=pl.ANY)
IN_VMEM = pl.BlockSpec(memory_space=pltpu.VMEM)


def dot_lanes(left, right):
    return lax.dot_general(left, right, (((1,), (1,)), ((), ())), preferred_element_type=F32)


def lanes(shape):
    return lax.broadcasted_iota(jnp.int32, shape, len(shape) - 1)


def swap_halves(tile):
    return pltpu.roll(tile, tile.shape[-1] // 2, 1)


class Gather:
    def __init__(self, index, own, slot, half, several, send, recv, here):
        z, s, y = here
        flip = lax.rem(s + 2, 4)
        other = s + 1 - 2 * lax.rem(s, 2)
        other_flip = lax.rem(other + 2, 4)
        self.near = [(z, flip, y), (z, s, 1 - y), (z, other, y)]
        self.mine, self.from_x, self.from_y, self.from_d = (s, y), (flip, y), (s, 1 - y), (flip, 1 - y)
        self.pair = [(other, y), (other_flip, y), (other, 1 - y), (other_flip, 1 - y)]
        self.index, self.own, self.slot, self.half = index, own, slot, half
        self.send, self.recv, self.several = send, recv, several

    def copy(self, step, src, dst, to):
        return pltpu.make_async_remote_copy(
            src_ref=src,
            dst_ref=dst,
            send_sem=self.send.at[self.index],
            recv_sem=self.recv.at[self.index, (0, 1, 3, 2, 2, 3, 3, 3)[step]],
            device_id=self.near[to],
            device_id_type=MESH,
        )

    def sends(self):
        mine, slot, half = self.slot(self.mine), self.slot, self.half
        return [
            (0, self.own, mine, 0),
            (1, self.own, mine, 1),
            (2, self.own, mine, 2),
            (3, half(self.from_x, 0), half(self.from_x, 0), 1),
            (4, half(self.from_y, 1), half(self.from_y, 1), 0),
            (5, slot(self.from_x), slot(self.from_x), 2),
            (6, slot(self.from_y), slot(self.from_y), 2),
            (7, slot(self.from_d), slot(self.from_d), 2),
        ]

    def begin(self, steps):
        for entry in self.sends():
            if entry[0] in steps:
                self.copy(*entry).start()

    def arrive(self, step):
        where = {
            0: lambda: self.slot(self.from_x),
            1: lambda: self.slot(self.from_y),
            2: lambda: self.several(4),
            3: lambda: self.slot(self.from_d),
        }[step]()
        self.copy(step, where, where, 0).wait_recv()

    def start(self):
        self.begin((0, 1, 2))

    def relay(self):
        self.arrive(0)
        self.begin((3, 5))
        self.arrive(1)
        self.begin((4, 6))

    def relay_far(self):
        self.arrive(3)
        self.begin((7,))

    def finish(self):
        self.arrive(2)

    def drain(self):
        sent = self.several(7)
        self.copy(0, sent, sent, 0).wait_send()


def fused_kernel(
    dims, factor,
    own_ref, w1_hbm, w2_hbm,
    ig_ref, parts,
    acts, deltas, cols, full, edge_s, edge_r, pack_s, pack_r, weight, shifted,
    facc, cacc, near, dl, dpos, zacc, igt, term_s, term_r,
    ag_s, ag_r, c1_s, c1_r, c1_l, c2_s, c2_r, g_s, g_r, h_s, h_r, t_s, t_r, w_sem,
):
    nch, nsx, nsy, rows, lx, ly, nz = dims
    g_ref, in_ref, act_ref = (own_ref.at[:, pl.ds(i * rows, rows)] for i in range(3))
    lane = ly * nz
    nk = nsx * nsy
    piece = rows * nch // nk
    sub = piece // 2
    npos = lx * lane
    wide = nsy * lane
    z, s, y = lax.axis_index("ch"), lax.axis_index("sx"), lax.axis_index("sy")
    here = (z, s, y)
    mine = s * nsy + y
    parity = lax.rem(z, 2)
    core = lax.rem(s, 2)
    turn = z // 2

    barrier = pltpu.get_barrier_semaphore()
    for step in range(1, nk):
        k = lax.rem(mine + step, nk)
        pl.semaphore_signal(
            barrier, inc=1, device_id=(z, k // nsy, lax.rem(k, nsy)), device_id_type=MESH
        )
    for step in range(1, nch):
        pl.semaphore_signal(
            barrier, inc=1, device_id=(lax.rem(z + step, nch), s, y), device_id_type=MESH
        )
    pl.semaphore_wait(barrier, nk - 1 + nch - 1)

    load_two = pltpu.make_async_copy(w2_hbm, weight, w_sem.at[0])
    load_two.start()
    load_one = pltpu.make_async_copy(w1_hbm, weight, w_sem.at[1])

    def block_copy(op, ref, q):
        dst_s, dst_y = 2 * (q // 2) + parity, q % 2
        src = ref.at[:, pl.ds(q * sub, sub)]
        dst = cols.at[op, turn, mine]
        remote = pltpu.make_async_remote_copy(
            src_ref=src, dst_ref=dst, send_sem=c1_s.at[op, q], recv_sem=c1_r.at[op, mine],
            device_id=(z, dst_s, dst_y), device_id_type=MESH,
        )
        local = pltpu.make_async_copy(src, dst, c1_l.at[op])
        same = jnp.logical_and(dst_s == s, dst_y == y)
        return same, local, remote

    def blocks_start(op, ref):
        for q in range(nk // 2):
            same, local, remote = block_copy(op, ref, q)

            @pl.when(same)
            def _():
                local.start()

            @pl.when(jnp.logical_not(same))
            def _():
                remote.start()

    def blocks_wait(op, ref):
        @pl.when(parity == core)
        def _():
            for step in range(1, nk):
                k = lax.rem(mine + step, nk)
                dst = cols.at[op, turn, k]
                pltpu.make_async_remote_copy(
                    src_ref=dst, dst_ref=dst, send_sem=c1_s.at[op, 0], recv_sem=c1_r.at[op, k],
                    device_id=here, device_id_type=MESH,
                ).wait_recv()
        for q in range(nk // 2):
            same, local, remote = block_copy(op, ref, q)

            @pl.when(same)
            def _():
                local.wait()

    def blocks_drain(op, ref):
        for q in range(nk // 2):
            same, local, remote = block_copy(op, ref, q)

            @pl.when(jnp.logical_not(same))
            def _():
                remote.wait_send()

    def spread_copy(op, step):
        block = cols.at[op, turn]
        return pltpu.make_async_remote_copy(
            src_ref=block, dst_ref=block, send_sem=c2_s.at[op, step - 1], recv_sem=c2_r.at[op, turn],
            device_id=(lax.rem(z + step, nch), s, y), device_id_type=MESH,
        )

    def spread_start(op):
        @pl.when(parity == core)
        def _():
            for step in range(1, nch):
                spread_copy(op, step).start()

    def spread_wait(op, t):
        @pl.when(core + 2 * t != z)
        def _():
            block = cols.at[op, t]
            pltpu.make_async_remote_copy(
                src_ref=block, dst_ref=block, send_sem=c2_s.at[op, 0], recv_sem=c2_r.at[op, t],
                device_id=here, device_id_type=MESH,
            ).wait_recv()

    def spread_drain(op):
        @pl.when(parity == core)
        def _():
            for step in range(1, nch):
                spread_copy(op, step).wait_send()

    def full_pass(hop, to):
        k = z - hop if to else z + hop
        valid = jnp.logical_and(k >= 0, z < nch - 1) if to else jnp.logical_and(k < nch, z > 0)
        k = jnp.clip(k, 0, nch - 1)
        copy = pltpu.make_async_remote_copy(
            src_ref=g_ref if hop == 0 else full.at[k], dst_ref=full.at[k],
            send_sem=g_s.at[hop, to], recv_sem=g_r.at[k],
            device_id=(jnp.clip(z + 2 * to - 1, 0, nch - 1), s, y), device_id_type=MESH,
        )
        return valid, copy

    def start_full(hop):
        for to in range(2):
            valid, copy = full_pass(hop, to)

            @pl.when(valid)
            def _():
                copy.start()

    def drain_full():
        for hop in range(nch - 1):
            for to in range(2):
                valid, copy = full_pass(hop, to)

                @pl.when(valid)
                def _():
                    copy.wait_send()

    def wait_full(hop):
        for k, valid in ((z - hop, z >= hop), (z + hop, z + hop < nch)):
            k = jnp.clip(k, 0, nch - 1)

            @pl.when(valid)
            def _():
                pltpu.make_async_remote_copy(
                    src_ref=full.at[k], dst_ref=full.at[k], send_sem=g_s.at[0, 0],
                    recv_sem=g_r.at[k], device_id=here, device_id_type=MESH,
                ).wait_recv()

    def whole(ref):
        slot = lambda k: ref.at[pl.ds(lx * k[0], lx), k[1]]
        half = lambda k, i: ref.at[pl.ds(lx * k[0] + i * (lx // 2), lx // 2), k[1]]
        several = lambda n: ref.at[pl.ds(0, lx * n // nsy)]
        return slot, half, several

    act_gather = Gather(0, act_ref, *whole(acts), ag_s, ag_r, here)
    delta_gather = Gather(1, dl, *whole(deltas), ag_s, ag_r, here)
    size = parts.shape[3]
    cut = size // 2 // 16 * 16

    def piece_gather(which, n):
        slot = lambda k: parts.at[which, n, k[0] * nsy + k[1]]
        half = lambda k, i: parts.at[
            which, n, k[0] * nsy + k[1], pl.ds(0, cut) if i == 0 else pl.ds(cut, size - cut)
        ]
        several = lambda count: parts.at[which, n, pl.ds(0, count)]
        return Gather(2 + 6 * which + n, slot((s, y)), slot, half, several, ag_s, ag_r, here)

    def clear():
        for t in range(2):
            for p in (0, nsx * lx + 1):
                shifted[t, p] = jnp.zeros(shifted.shape[2:], BF16)
        facc[...] = jnp.zeros(facc.shape, F32)
        for b in range(3):
            for x in range(lx + 2):
                cacc[b, x] = jnp.zeros(cacc.shape[2:], F32)
        zacc[...] = jnp.zeros(zacc.shape, F32)
        acts[pl.ds(lx * s, lx), y] = act_ref[...]
        full[z] = g_ref[...]

    def shift_columns(op, t):
        @pl.loop(0, nsx * lx)
        def _(p):
            owner, inner = p // lx, lax.rem(p, lx)
            tiles = [cols[op, t, owner * nsy + j, inner] for j in range(nsy)]
            plane = jnp.concatenate(tiles, axis=1).astype(F32)
            where = lanes((sub, wide))
            row, depth = where // nz, lax.rem(where, nz)
            for b in range(3):
                for c in range(3):
                    move = (nz * (b - 1) + c - 1) % wide
                    value = pltpu.roll(plane, move, 1) if move else plane
                    keep = where >= 0
                    if b == 0:
                        keep = jnp.logical_and(keep, row < nsy * ly - 1)
                    if b == 2:
                        keep = jnp.logical_and(keep, row > 0)
                    if c == 0:
                        keep = jnp.logical_and(keep, depth < nz - 1)
                    if c == 2:
                        keep = jnp.logical_and(keep, depth > 0)
                    value = jnp.where(keep, value, 0.0).astype(BF16)
                    for j in range(nsy):
                        shifted[t, p + 1, j, pl.ds((3 * b + c) * sub, sub)] = value[
                            :, j * lane : (j + 1) * lane
                        ]

    def filter_pieces(which, left, t, first=0, last=3):
        @pl.loop(first, last)
        def _(a):
            facc[:, :rows] = jnp.zeros((facc.shape[0], rows), F32)

            @pl.loop(0, nsx)
            def _(o):
                cells = shifted[t, pl.ds(2 - a + lx * o, lx)]
                other = left[pl.ds(lx * o, lx)]
                cells = jnp.concatenate([cells[i, j] for i in range(lx) for j in range(nsy)], axis=1)
                other = jnp.concatenate([other[i, j] for i in range(lx) for j in range(nsy)], axis=1)
                facc[:, :rows] += dot_lanes(cells, other)

            group = 9 * sub
            n = 3 * t + a
            parts[which, n, mine, pl.ds(0, group)] = (facc[:, :lane] * factor).astype(BF16)
            for low, high, size_of, to in ((0, 4 * sub, 4 * sub, 0), (8 * sub, 17 * sub // 2, sub // 2, 4 * sub)):
                first = facc[pl.ds(low, size_of), lane : 2 * lane] * factor
                second = facc[pl.ds(high, size_of), lane : 2 * lane] * factor
                both = jnp.where(lanes(first.shape) < rows - lane, first, swap_halves(second))
                parts[which, n, mine, pl.ds(group + to, size_of)] = both.astype(BF16)
            piece_gather(which, n).start()

    def relay_pieces(which, t):
        @pl.loop(0, 3)
        def _(a):
            piece_gather(which, 3 * t + a).relay()

    def far_pieces(which, t):
        @pl.loop(0, 3)
        def _(a):
            piece_gather(which, 3 * t + a).relay_far()

    def finish_pieces(which):
        @pl.loop(0, 6)
        def _(n):
            piece_gather(which, n).finish()

    low_half = lanes((rows, lane)) < nz

    left_dev = (z, lax.rem(s + nsx - 1, nsx), y)
    right_dev = (z, lax.rem(s + 1, nsx), y)

    def halo(i, src, dst, dev):
        return pltpu.make_async_remote_copy(
            src_ref=src, dst_ref=dst, send_sem=h_s.at[i], recv_sem=h_r.at[i],
            device_id=dev, device_id_type=MESH,
        )

    to_y = halo(0, pack_s, pack_r, (z, s, 1 - y))
    to_left = halo(1, edge_s.at[0], edge_r.at[1], left_dev)
    to_right = halo(2, edge_s.at[1], edge_r.at[0], right_dev)
    has_left, has_right = s > 0, s < nsx - 1

    def term_copy(step):
        to = lax.rem(z + step, nch)
        return pltpu.make_async_remote_copy(
            src_ref=term_s.at[to], dst_ref=term_r.at[z], send_sem=t_s.at[step - 1],
            recv_sem=t_r.at[z], device_id=(to, s, y), device_id_type=MESH,
        )

    def act_grad():
        load_two.wait()

        @pl.loop(0, 9)
        def _(ab):
            a, b = ab // 3, lax.rem(ab, 3)
            left = weight[pl.ds(3 * ab, 3)].reshape(3 * rows, nch * rows)
            right = jnp.concatenate(
                [jnp.concatenate([full[k, x] for x in range(lx)], axis=1) for k in range(nch)], axis=0
            )
            value = jnp.dot(left, right, preferred_element_type=F32)
            for x in range(lx):
                cacc[b, a + x] += value[:, x * lane : (x + 1) * lane]

        load_one.start()

    def fold_halo():
        depth = lax.rem(lanes((rows, lane)), nz)
        low = None
        for x in range(lx + 2):
            sums = []
            for b in range(3):
                total = cacc[b, x, pl.ds(rows, rows)]
                back = pltpu.roll(cacc[b, x, pl.ds(0, rows)], lane - 1, 1)
                ahead = pltpu.roll(cacc[b, x, pl.ds(2 * rows, rows)], 1, 1)
                total += jnp.where(depth < nz - 1, back, 0.0)
                total += jnp.where(depth > 0, ahead, 0.0)
                sums.append(total)
            up, down = swap_halves(sums[0]), swap_halves(sums[2])
            near[x] = sums[1] + jnp.where(low_half, up, down)
            if x % 2 == 0:
                low = jnp.where(y == 0, down, sums[0])
            else:
                high = jnp.where(y == 0, sums[2], up)
                pack_s[x // 2] = jnp.where(low_half, low, high).astype(BF16)
        to_y.start()

    def fold_edges():
        to_y.wait_recv()
        for x in range(lx + 2):
            value = pack_r[x // 2].astype(F32)
            turned = swap_halves(value)
            to_high, to_low = (turned, value) if x % 2 == 0 else (value, turned)
            high = jnp.where(low_half, 0.0, to_high)
            low = jnp.where(low_half, to_low, 0.0)
            near[x] += jnp.where(y == 0, high, low)
        edge_s[0] = near[0].astype(BF16)
        edge_s[1] = near[lx + 1].astype(BF16)

        @pl.when(has_left)
        def _():
            to_left.start()

        @pl.when(has_right)
        def _():
            to_right.start()

    def make_delta():
        @pl.when(has_right)
        def _():
            to_left.wait_recv()
            near[lx] += edge_r[1].astype(F32)

        @pl.when(has_left)
        def _():
            to_right.wait_recv()
            near[1] += edge_r[0].astype(F32)

        for x in range(lx):
            total = jnp.where(act_ref[x].astype(F32) > 0.0, near[x + 1], 0.0).astype(BF16)
            dl[x] = total
            deltas[lx * s + x, y] = total
        delta_gather.start()

    def place_delta():
        for x in range(lx + 2):
            place = lx * s + x - 1
            inside = jnp.logical_and(place >= 0, place < nsx * lx)
            place = jnp.clip(place, 0, nsx * lx - 1)
            own = deltas[place, y].astype(F32).T
            beside = deltas[place, 1 - y].astype(F32).T
            own = jnp.where(inside, own, 0.0).astype(BF16)
            beside = jnp.where(inside, jnp.where(y == 0, beside[:nz], beside[lane - nz :]), 0.0)
            dpos[x, 0] = jnp.where(y == 0, 0.0, beside).astype(BF16)
            for j in range(ly):
                dpos[x, 1 + j] = own[j * nz : (j + 1) * nz]
            dpos[x, ly + 1] = jnp.where(y == 0, beside, 0.0).astype(BF16)

    def input_terms(first, last):
        @pl.loop(first, last)
        def _(ab):
            a, b = ab // 3, lax.rem(ab, 3)
            left = dpos[pl.ds(2 - a, lx), pl.ds(2 - b, ly)].reshape(npos, rows)
            for c in range(3):
                zacc[c] += jnp.dot(left, weight[3 * ab + c], preferred_element_type=F32)

    def pack_terms():
        for i in range(npos // nz):
            span = slice(i * nz, (i + 1) * nz)
            total = zacc[1, span]
            at = lax.broadcasted_iota(jnp.int32, total.shape, 0)
            total += jnp.where(at < nz - 1, pltpu.roll(zacc[0, span], nz - 1, 0), 0.0)
            total += jnp.where(at > 0, pltpu.roll(zacc[2, span], 1, 0), 0.0)
            igt[span] = total.astype(BF16)

        for k in range(nch):
            shape = (rows, nch * rows)
            pick = lanes(shape) == lax.broadcasted_iota(jnp.int32, shape, 0) + k * rows
            value = dot_lanes(pick.astype(BF16), igt[...]).astype(BF16)
            for x in range(lx):
                term_s[k, x] = value[:, x * lane : (x + 1) * lane]

    def send_terms():
        for step in range(1, nch):
            term_copy(step).start()

    def sum_terms():
        total = term_s[z].astype(F32)
        for step in range(1, nch):
            k = lax.rem(z + step, nch)
            pltpu.make_async_remote_copy(
                src_ref=term_r.at[k], dst_ref=term_r.at[k], send_sem=t_s.at[0], recv_sem=t_r.at[k],
                device_id=here, device_id_type=MESH,
            ).wait_recv()
            total += term_r[k].astype(F32)
        ig_ref[...] = total.astype(BF16)

    def drain_columns():
        for op, ref in ((0, g_ref), (1, in_ref)):
            blocks_drain(op, ref)
            spread_drain(op)
        drain_full()

    def drain_halo():
        for step in range(1, nch):
            term_copy(step).wait_send()
        to_y.wait_send()

        @pl.when(has_left)
        def _():
            to_left.wait_send()

        @pl.when(has_right)
        def _():
            to_right.wait_send()

        act_gather.drain()
        delta_gather.drain()

    def drain_pieces(which):
        @pl.loop(0, 6)
        def _(n):
            piece_gather(which, n).drain()

    blocks_start(0, g_ref)
    act_gather.start()
    start_full(0)
    blocks_wait(0, g_ref)
    spread_start(0)
    clear()
    act_gather.relay()
    blocks_start(1, in_ref)

    @pl.when(parity == core)
    def _():
        shift_columns(0, turn)

    act_gather.relay_far()
    act_gather.finish()

    @pl.when(parity != core)
    def _():
        spread_wait(0, turn)
        shift_columns(0, turn)

    filter_pieces(0, acts, turn)
    spread_wait(0, 1 - turn)
    wait_full(1)
    start_full(1)
    shift_columns(0, 1 - turn)
    filter_pieces(0, acts, 1 - turn, 0, 1)
    wait_full(2)
    start_full(2)
    filter_pieces(0, acts, 1 - turn, 1, 3)
    relay_pieces(0, turn)
    blocks_wait(1, in_ref)
    wait_full(3)
    spread_start(1)
    act_grad()
    fold_halo()
    fold_edges()
    make_delta()
    relay_pieces(0, 1 - turn)
    far_pieces(0, turn)
    delta_gather.relay()
    spread_wait(1, turn)
    shift_columns(1, turn)
    delta_gather.relay_far()
    spread_wait(1, 1 - turn)
    shift_columns(1, 1 - turn)
    delta_gather.finish()
    filter_pieces(1, deltas, turn)
    far_pieces(0, 1 - turn)
    place_delta()
    load_one.wait()
    input_terms(0, 9)
    pack_terms()
    send_terms()
    relay_pieces(1, turn)
    filter_pieces(1, deltas, 1 - turn)
    finish_pieces(0)
    drain_columns()
    drain_pieces(0)
    relay_pieces(1, 1 - turn)
    far_pieces(1, turn)
    far_pieces(1, 1 - turn)
    sum_terms()
    drain_halo()
    finish_pieces(1)
    drain_pieces(1)


def join_kernel(dims, parts, out_two, out_one):
    nch, nsx, nsy, rows, lx, ly, nz = dims
    lane = ly * nz
    nk = nsx * nsy
    sub = rows * nch // nk // 2
    group = 9 * sub
    rest = rows - lane
    a = pl.program_id(0) // 3
    shape = (lane, lane)
    same = (lanes(shape) == lax.broadcasted_iota(jnp.int32, shape, 0)).astype(BF16)
    shape = (rest, lane)
    down, across = lax.broadcasted_iota(jnp.int32, shape, 0), lanes(shape)
    picks = [(across == down).astype(BF16), (across == down + rest).astype(BF16)]
    shape = (sub, lane)
    own_half = lax.broadcasted_iota(jnp.int32, shape, 0) // (sub // 2) == lanes(shape) // rest

    def gathered(which, load):
        found = []
        for k in range(nch):
            for q in range(nk // 2):
                slot = (2 * (q // 2) + k % 2) * nsy + q % 2
                found.append(load((which, 3 * (k // 2) + a, slot)))
        return jnp.concatenate(found, axis=0)

    def join(b, c, which, out):
        block = 3 * b + c
        out[:lane] = dot_lanes(same, gathered(which, lambda at: parts[(*at, pl.ds(block * sub, sub))]))
        start = group + block % 4 * sub
        if block < 8:
            tail = gathered(which, lambda at: parts[(*at, pl.ds(start, sub))])
            out[lane:] = dot_lanes(picks[block // 4], tail)
        else:
            def load(at):
                half = parts[(*at, pl.ds(group + 4 * sub, sub // 2))].astype(F32)
                both = jnp.concatenate([half, half], axis=0)
                return jnp.where(own_half, both, 0.0).astype(BF16)

            out[lane:] = dot_lanes(picks[0] + picks[1], gathered(which, load))

    for b in range(3):
        @pl.when(lax.rem(pl.program_id(0), 3) == b)
        def _():
            for c in range(3):
                join(b, c, 0, out_two.at[c])
                join(b, c, 1, out_one.at[2 - c])


def tiles(array):
    rows, lx, ly, nz = array.shape
    return array.reshape(rows, lx, ly * nz).transpose(1, 0, 2)


def fused_shards(inputs, pre_act, out_grad, weight_one, weight_two):
    rows, lx, ly, nz = pre_act.shape
    nch, nsx, nsy = (lax.axis_size(axis) for axis in ("ch", "sx", "sy"))
    dims = (nch, nsx, nsy, rows, lx, ly, nz)
    lane = ly * nz
    nk = nsx * nsy
    channels = nch * rows
    piece = channels // nk
    npos = lx * lane
    factor = 1.0 / math.sqrt(npos * nk)
    size = 9 * piece // 2 * rows // lane
    planes = nsx * lx
    tile = (lx, rows, lane)
    vm = lambda *shape: pltpu.VMEM(shape, BF16)
    dma = lambda *shape: pltpu.SemaphoreType.DMA(shape)
    active = jnp.maximum(pre_act, jnp.zeros((), pre_act.dtype))
    own = tiles(jnp.concatenate([out_grad, inputs, active], axis=0))
    grad, pieces = pl.pallas_call(
        functools.partial(fused_kernel, dims, factor),
        out_shape=(
            jax.ShapeDtypeStruct(tile, BF16),
            pltpu.VMEM((2, 6, nk, size, lane), BF16),
        ),
        in_specs=[IN_VMEM] + [ANY] * 2,
        out_specs=(IN_VMEM, IN_VMEM),
        scratch_shapes=[
            vm(planes, nsy, rows, lane),
            vm(planes, nsy, rows, lane),
            vm(2, 2, nk, lx, piece // 2, lane),
            vm(nch, lx, rows, lane),
            vm(2, rows, lane),
            vm(2, rows, lane),
            vm(lx // 2 + 1, rows, lane),
            vm(lx // 2 + 1, rows, lane),
            vm(27, rows, channels),
            vm(2, planes + 2, nsy, 9 * piece // 2, lane),
            pltpu.VMEM((9 * piece // 2, 2 * lane), F32),
            pltpu.VMEM((3, lx + 2, 3 * rows, lane), F32),
            pltpu.VMEM((lx + 2, rows, lane), F32),
            vm(lx, rows, lane),
            vm(lx + 2, ly + 2, nz, rows),
            pltpu.VMEM((3, npos, channels), F32),
            vm(npos, channels),
            vm(nch, lx, rows, lane),
            vm(nch, lx, rows, lane),
            dma(14), dma(14, 4), dma(2, nk // 2), dma(2, nk), dma(2),
            dma(2, nch - 1), dma(2, 2), dma(nch - 1, 2), dma(nch),
            dma(3), dma(3), dma(nch - 1), dma(nch), dma(2),
        ],
        compiler_params=pltpu.CompilerParams(
            collective_id=0, has_side_effects=True, vmem_limit_bytes=42 * 1024 * 1024
        ),
    )(own, weight_one, weight_two)
    two, one = pl.pallas_call(
        functools.partial(join_kernel, dims),
        grid=(9,),
        out_shape=(jax.ShapeDtypeStruct((27, rows, channels), F32),) * 2,
        in_specs=[IN_VMEM],
        out_specs=(
            pl.BlockSpec((3, rows, channels), lambda n: (n, 0, 0)),
            pl.BlockSpec((3, rows, channels), lambda n: (8 - n, 0, 0)),
        ),
        compiler_params=pltpu.CompilerParams(vmem_limit_bytes=20 * 1024 * 1024),
    )(pieces)
    grad = grad.transpose(1, 0, 2).reshape(rows, lx, ly, nz)
    return grad, one, two


def fits(mesh, rows, lx, ly, nz):
    nch, nsx, nsy = (mesh.shape[axis] for axis in ("ch", "sx", "sy"))
    return (
        (nch, nsx, nsy) == (4, 4, 2)
        and lx % 4 == 0
        and ly == 2
        and ly * nz == 128
        and rows % 64 == 0
        and 128 < rows < 256
    )


def solution(mesh):
    in_specs = (
        P("ch", "sx", "sy", None),
        P("ch", "sx", "sy", None),
        P("ch", "sx", "sy", None),
        P(None, "ch", None),
        P(None, "ch", None),
    )
    out_specs = (P("ch", "sx", "sy", None), P(None, "ch", None), P(None, "ch", None))

    def body(*args):
        return (fused_shards if fits(mesh, *args[1].shape) else shards)(*args)

    return jax.shard_map(body, mesh=mesh, in_specs=in_specs, out_specs=out_specs, check_vma=False)
```
